512 devices in a mesh: band: 32 (over x_lo, z, core), grid: 16 (over x_hi, y).
Axes of the slice: x: 4 (x_hi: 2, x_lo: 2; x = x_hi * 2 + x_lo), y: 8, z: 8, core: 2. Of those that a mesh axis runs over, the one named last changes fastest.
Arguments:
- orbitals: float32 [32, 48, 2304], P('band', 'grid'), may hold values from -6 to 6
Outputs:
- compressed: float32 [32, 48, 2304], P('band', 'grid')
The draws below stay inside these ranges and needn't reach their ends.
All inputs are finite; a program needn't handle non-finite values.
Results may differ from the reference program's by a relative error of at most 0.000092.
Values sent between devices are 32-bit elements; how exact they have to be, the bound alone decides.
No kernel may reach another device: no remote copies, remote signals or barrier semaphores. Data moves between devices by JAX's collectives and lax.ppermute only.
A program may use at most 64 MiB of HBM per device.

```python
import jax
import jax.numpy as jnp
from jax import lax

NG = 48
BANDS = 32


def shard_levels(own_key, shape, pieces, least, top_value):
    level = 1.0
    for dim, blocks in pieces:
        steps = jax.random.uniform(jax.random.fold_in(jax.random.fold_in(own_key, 6), dim), (blocks,), jnp.float32, least / len(pieces), top_value / len(pieces))
        level = level * jnp.repeat(jnp.exp(steps), shape[dim] // blocks).reshape((-1,) + (1,) * (len(shape) - 1 - dim))
    return level


def centred(stream_key, shape, scale, limit, pieces=(), held_as=jnp.bfloat16):
    array = jax.random.normal(stream_key, shape, jnp.float32) * scale
    if len(pieces) > 0:
        array = shard_levels(stream_key, shape, pieces, -0.22, 0.18) * array
    return jnp.clip(array, min=-limit, max=limit).astype(held_as)


def setup_inputs(seed: int = 0) -> dict:
    seeds = jax.random.split(jax.random.key(seed), 2)
    orbitals = centred(seeds[0], (BANDS, NG, NG * NG), 1.0, 6.0, ((0, 32), (1, 16)), jnp.float32)
    return {"orbitals": orbitals}


coulomb_scale = 50.0

def coulomb_table(length):
    counter = jnp.arange(length, dtype=jnp.int32)
    signed = jnp.where(counter < length // 2, counter, counter - length).astype(jnp.float32)
    squares = signed * signed
    summed = squares[:, None, None] + squares[None, :, None] + squares[None, None, :]
    return jnp.where(summed > 0.0, coulomb_scale / jnp.maximum(summed, 1.0), 0.0)

def reference(orbitals):
    band_count = orbitals.shape[0]
    length = orbitals.shape[1]
    fields = orbitals.reshape(band_count, length, length, length)
    kernel = coulomb_table(length)

    def apply_one(orbital):
        density = orbital[None] * fields
        spectrum = jnp.fft.fftn(density, axes=(1, 2, 3))
        potential = jnp.real(jnp.fft.ifftn(spectrum * kernel, axes=(1, 2, 3)))
        return -jnp.sum(fields * potential, axis=0)
    exchange = lax.map(apply_one, fields)
    flat_orbitals = fields.reshape(band_count, -1)
    flat_exchange = exchange.reshape(band_count, -1)
    cells_total = float(length ** 3)
    projected = jnp.dot(flat_orbitals.astype(jnp.float32), flat_exchange.T.astype(jnp.float32), precision=lax.Precision.HIGHEST, preferred_element_type=jnp.float32) / cells_total
    definite = -0.5 * (projected + projected.T)
    lower = jnp.linalg.cholesky(definite)
    inverse_lower = jax.scipy.linalg.solve_triangular(lower, jnp.eye(band_count, dtype=jnp.float32), lower=True)
    compressed = jnp.dot(inverse_lower.astype(jnp.float32), flat_exchange.astype(jnp.float32), precision=lax.Precision.HIGHEST, preferred_element_type=jnp.float32)
    return compressed.reshape(orbitals.shape)
```

```python
import math

import jax
import jax.numpy as jnp
import numpy as np
from jax import lax
from jax.experimental import pallas as pl
from jax.experimental.pallas import tpu as pltpu
from jax.sharding import Mesh, PartitionSpec as P

NG = 48
BANDS = 32
COULOMB = 50.0
SLABS = 16
PLANES = NG // SLABS
COLS = NG * NG // 128
ROWS = 56
USED = PLANES * COLS
CHIPS = BANDS // 2
BAND, GRID = ("xl", "z", "c"), ("xh", "y")
PAIR = ("xl", "z")
f32, bf16 = jnp.float32, jnp.bfloat16


def real_basis():
    half = NG // 2
    freq = np.concatenate([np.arange(half + 1), np.arange(1, half)])
    turn = 2.0 * np.pi * ((freq[:, None] * np.arange(NG)[None, :]) % NG) / NG
    wave = np.where(np.arange(NG)[:, None] <= half, np.cos(turn), np.sin(turn))
    norm = np.where((np.arange(NG) == 0) | (np.arange(NG) == half), 1.0, 2.0) / NG
    return wave * np.sqrt(norm)[:, None], freq.astype(np.float64) ** 2


def halves(matrix):
    high = matrix.astype(np.float32).astype(bf16)
    low = (matrix - high.astype(np.float64)).astype(np.float32).astype(bf16)
    return high, low


def from_left(matrix):
    high, low = halves(matrix)
    return np.concatenate([high, high, low], 1)


BASIS, SQUARES = real_basis()
BASIS_X = BASIS[:, [PLANES * (r % SLABS) + r // SLABS for r in range(NG)]]
LEFTS = np.stack([from_left(m) for m in (BASIS_X, BASIS, BASIS.T, BASIS_X.T)])


def last_edge():
    wide = np.zeros((2, NG, 128))
    wide[0, :, :NG] = BASIS.T
    wide[1, :, 64 : 64 + NG] = BASIS.T
    return halves(wide)


LAST_HIGH, LAST_LOW = last_edge()


def split(x):
    high = x.astype(bf16)
    return high, (x - high.astype(f32)).astype(bf16)


def dot(a, b):
    return jnp.dot(a, b, preferred_element_type=f32)


def dot_t(a, b):
    return lax.dot_general(a, b, (((1,), (1,)), ((), ())), preferred_element_type=f32)


def left_mul(matrix, x):
    high, low = split(x)
    return dot(matrix, jnp.concatenate([high, low, high], 0))


def tables_kernel(high_ref, low_ref, wide_high, wide_low, coulomb):
    wide_high[...] = jnp.zeros_like(wide_high)
    wide_low[...] = jnp.zeros_like(wide_low)
    for w in range(2):
        for d in range(2):
            for i in range(4):
                rows = slice(48 * i + 64 * w, 48 * i + 64 * w + 48)
                cols = slice(128 * i, 128 * i + 128)
                wide_high[w, d, rows, cols] = high_ref[d]
                wide_low[w, d, rows, cols] = low_ref[d]

    def square(i):
        freq = jnp.where(i <= NG // 2, i, i - NG // 2).astype(f32)
        return freq * freq

    middle = lax.broadcasted_iota(jnp.int32, (NG, 128), 0)
    lane = lax.broadcasted_iota(jnp.int32, (NG, 128), 1)
    last = jnp.minimum(jnp.where(lane >= 64, lane - 64, lane), NG - 1)
    rest = square(middle) + square(last)
    for k in range(NG):
        total = rest + float(SQUARES[k])
        coulomb[k] = jnp.where(total > 0.0, -COULOMB / jnp.maximum(total, 1.0), 0.0)


def tables():
    wide = jax.ShapeDtypeStruct((2, 2, 256, 512), bf16)
    return pl.pallas_call(
        tables_kernel,
        out_shape=(wide, wide, jax.ShapeDtypeStruct((NG, NG, 128), f32)),
        name="tables",
    )(jnp.asarray(LAST_HIGH), jnp.asarray(LAST_LOW))


def exchange_kernel(
    own_ref, pair_ref, left_ref, wide_high, wide_low, coulomb, out_ref, rho_h, rho_l, za, zb, sol_h, sol_l
):
    def column(ref, first, c):
        return jnp.concatenate(
            [ref[pl.ds(first + COLS * p + c, SLABS, stride=ROWS), :] for p in range(PLANES)], 0
        )

    def place(c):
        return slice(48 * (c // 3), 48 * (c // 3) + 48), slice(128 * (c % 3), 128 * (c % 3) + 128)

    for c in range(COLS):
        own = column(own_ref, 0, c)
        rows, cols = place(c)
        for d in range(2):
            high, low = split(own * column(pair_ref, d * SLABS * ROWS, c))
            rho_h[d, rows, cols] = high
            rho_l[d, rows, cols] = low
    for w in range(2):
        window = slice(128 * w, 128 * w + 256)
        out = None
        for d in range(2):
            high, low = rho_h[d, :, window], rho_l[d, :, window]
            term = dot(high, wide_high[w, d]) + dot(low, wide_high[w, d]) + dot(high, wide_low[w, d])
            out = term if out is None else out + term
        for c in range(6):
            for i in range(4):
                y = 8 * c + 4 * w + i
                za[48 * y : 48 * y + 48, :] = out[48 * c : 48 * c + 48, 128 * i : 128 * i + 128]
    for y in range(0, NG, 2):
        both = jnp.concatenate([za[48 * y : 48 * y + 48, :], za[48 * y + 48 : 48 * y + 96, :]], 1)
        both = left_mul(left_ref[0], both)
        zb[48 * y : 48 * y + 48, :] = both[:, :128]
        zb[48 * y + 48 : 48 * y + 96, :] = both[:, 128:]
    for k in range(0, NG, 2):
        both = jnp.concatenate([zb[pl.ds(k, 48, stride=48), :], zb[pl.ds(k + 1, 48, stride=48), :]], 1)
        both = left_mul(left_ref[1], both) * jnp.concatenate([coulomb[k], coulomb[k + 1]], 1)
        both = left_mul(left_ref[2], both)
        za[pl.ds(k, 48, stride=48), :] = both[:, :128]
        za[pl.ds(k + 1, 48, stride=48), :] = both[:, 128:]
    for y in range(0, NG, 2):
        both = jnp.concatenate([za[48 * y : 48 * y + 48, :], za[48 * y + 48 : 48 * y + 96, :]], 1)
        both = left_mul(left_ref[3], both)
        for e in range(2):
            c, w, i = (y + e) // 8, ((y + e) % 8) // 4, (y + e) % 4
            high, low = split(both[:, 128 * e : 128 * e + 128])
            sol_h[w, 48 * c : 48 * c + 48, 128 * i : 128 * i + 128] = high
            sol_l[w, 48 * c : 48 * c + 48, 128 * i : 128 * i + 128] = low
    thirds = []
    for d in range(2):
        a, b = [
            dot_t(sol_h[w], wide_high[w, d]) + dot_t(sol_l[w], wide_high[w, d]) + dot_t(sol_h[w], wide_low[w, d])
            for w in range(2)
        ]
        thirds.append((a[:, :128], a[:, 128:] + b[:, :128], b[:, 128:]))
    for c in range(COLS):
        rows, _ = place(c)
        out = thirds[0][c % 3][rows] * column(pair_ref, 0, c)
        out = out + thirds[1][c % 3][rows] * column(pair_ref, SLABS * ROWS, c)
        for p in range(PLANES):
            out_ref[pl.ds(COLS * p + c, SLABS, stride=ROWS), :] = out[16 * p : 16 * p + 16]
    for r in range(USED, ROWS):
        out_ref[pl.ds(r, SLABS, stride=ROWS), :] = jnp.zeros((SLABS, 128), f32)


def partial_exchange(own, pair, made):
    big = pltpu.VMEM((NG * NG, 128), f32)
    rho, solved = pltpu.VMEM((2, 288, 384), bf16), pltpu.VMEM((2, 288, 512), bf16)
    return pl.pallas_call(
        exchange_kernel,
        out_shape=jax.ShapeDtypeStruct((SLABS * ROWS, 128), f32),
        scratch_shapes=[rho, rho, big, big, solved, solved],
        name="exchange",
    )(own, pair, jnp.asarray(LEFTS), *made)


def projected_kernel(orbital_ref, field_ref, out_ref):
    def flat(ref):
        return jnp.concatenate([ref[pl.ds(r, BANDS, stride=ROWS), :] for r in range(USED)], 1)

    left_h, left_l = split(flat(orbital_ref))
    right_h, right_l = split(flat(field_ref))
    out = dot_t(left_h, right_h) + dot_t(left_l, right_h) + dot_t(left_h, right_l)
    out_ref[...] = jnp.concatenate([out[8 * q : 8 * q + 8, :] for q in range(4)], 1)


def projected_part(orbitals, fields):
    return pl.pallas_call(
        projected_kernel, out_shape=jax.ShapeDtypeStruct((8, 128), f32), name="projected"
    )(orbitals, fields)


BLOCK = 4


def place_of(band):
    return (band % 2) * CHIPS + band // 2


def finish_kernel(band_ref, parts_ref, field_ref, out_ref, flat):
    band = band_ref[0]
    packed = jnp.sum(parts_ref[...], axis=0)
    matrix = jnp.concatenate([packed[:, 32 * q : 32 * q + 32] for q in range(4)], 0)
    definite = (matrix + matrix.T) * (-0.5 / float(NG**3))
    row = lax.broadcasted_iota(jnp.int32, (BANDS, 2 * BANDS), 0)
    lane = lax.broadcasted_iota(jnp.int32, (BANDS, 2 * BANDS), 1)
    order = 2 * (row % CHIPS) + row // CHIPS
    unit = jnp.where(row[:, :BANDS] == lane[:, :BANDS], 1.0, 0.0).astype(f32)
    state = jnp.concatenate([definite, unit], 1)
    for first in range(0, BANDS, BLOCK):
        at = [place_of(first + i) for i in range(BLOCK)]
        columns = [jnp.broadcast_to(state[:, a : a + 1], (BANDS, 2 * BANDS)) for a in at]
        pivots = [state[a : a + 1, :] for a in at]
        for i in range(BLOCK):
            factor = jnp.where(order > first + i, columns[i] / columns[i][at[i] : at[i] + 1, :], 0.0)
            for j in range(i + 1, BLOCK):
                columns[j] = columns[j] - factor * columns[j][at[i] : at[i] + 1, :]
                pivots[j] = pivots[j] - factor[at[j] : at[j] + 1, :] * pivots[i]
            state = state - factor * pivots[i]
    mine = (band % 2) * CHIPS + band // 2
    picked = jnp.sum(jnp.where(row == mine, state, 0.0), axis=0, keepdims=True)
    pivot = jnp.sum(jnp.where(lane[:1] == mine, picked, 0.0), axis=1, keepdims=True)
    weights = picked * lax.rsqrt(pivot)
    total = None
    for k in range(BANDS):
        weight = weights[:, BANDS + k : BANDS + k + 1]
        term = weight * field_ref[ROWS * k : ROWS * k + ROWS, :]
        total = term if total is None else total + term
    flat[...] = total
    for c in range(COLS):
        out_ref[:, 128 * c : 128 * c + 128] = flat[pl.ds(c, PLANES, stride=COLS), :]


def finish(band, parts, fields):
    vmem = pl.BlockSpec(memory_space=pltpu.VMEM)
    return pl.pallas_call(
        finish_kernel,
        out_shape=jax.ShapeDtypeStruct((PLANES, NG * NG), f32),
        in_specs=[pl.BlockSpec(memory_space=pltpu.SMEM), vmem, vmem],
        scratch_shapes=[pltpu.VMEM((ROWS, 128), f32)],
        name="finish",
    )(band, parts, fields)


def to_everyone(tile, devices, axis):
    return lax.all_to_all(jnp.broadcast_to(tile[None], (devices, *tile.shape)), axis, 0, 0, tiled=True)


def of_every_band(tile):
    chips = to_everyone(tile, CHIPS, PAIR)
    return lax.all_gather(chips, "c", axis=0, tiled=False).reshape(BANDS * ROWS, 128)


def per_device(orbitals):
    tile = jnp.pad(orbitals.reshape(USED, 128), ((0, ROWS - USED), (0, 0)))
    made = tables()
    moves = [
        (b * SLABS + s, (2 * s + b % 2) * SLABS + b // 2) for b in range(BANDS) for s in range(SLABS)
    ]
    partner = lax.ppermute(tile, BAND + GRID, moves)
    own = to_everyone(tile, SLABS, GRID).reshape(SLABS * ROWS, 128)
    pair = of_every_band(partner)
    partial = partial_exchange(own, pair, made)
    all_orbitals = of_every_band(tile)
    shares = lax.all_to_all(partial.reshape(SLABS, ROWS, 128), GRID, 0, 0, tiled=True)
    field = jnp.sum(shares, axis=0)
    all_fields = of_every_band(field)
    parts = to_everyone(projected_part(all_orbitals, all_fields), SLABS, GRID)
    band = lax.axis_index(BAND).astype(jnp.int32).reshape(1)
    return finish(band, parts, all_fields).reshape(1, PLANES, NG * NG)


def solution(mesh):
    parted = Mesh(mesh.devices.reshape(2, 8, 2, 2, 8), BAND + GRID)
    spec = P(BAND, GRID, None)
    return jax.shard_map(per_device, mesh=parted, in_specs=(spec,), out_specs=spec, check_vma=False)
```

```python
import math

import jax
import jax.numpy as jnp
import numpy as np
from jax import lax
from jax.experimental import pallas as pl
from jax.experimental.pallas import tpu as pltpu
from jax.sharding import Mesh, PartitionSpec as P

NG = 48
BANDS = 32
COULOMB = 50.0
SLABS = 16
PLANES = NG // SLABS
COLS = NG * NG // 128
ROWS = 56
USED = PLANES * COLS
CHIPS = BANDS // 2
BAND, GRID = ("xl", "z", "c"), ("xh", "y")
PAIR = ("xl", "z")
f32, bf16 = jnp.float32, jnp.bfloat16


def real_basis():
    half = NG // 2
    freq = np.concatenate([np.arange(half + 1), np.arange(1, half)])
    turn = 2.0 * np.pi * ((freq[:, None] * np.arange(NG)[None, :]) % NG) / NG
    wave = np.where(np.arange(NG)[:, None] <= half, np.cos(turn), np.sin(turn))
    norm = np.where((np.arange(NG) == 0) | (np.arange(NG) == half), 1.0, 2.0) / NG
    return wave * np.sqrt(norm)[:, None], freq.astype(np.float64) ** 2


def halves(matrix):
    high = matrix.astype(np.float32).astype(bf16)
    low = (matrix - high.astype(np.float64)).astype(np.float32).astype(bf16)
    return high, low


def from_left(matrix):
    high, low = halves(matrix)
    return np.concatenate([high, high, low], 1)


BASIS, SQUARES = real_basis()
BASIS_X = BASIS[:, [PLANES * (r % SLABS) + r // SLABS for r in range(NG)]]
LEFTS = np.stack([from_left(m) for m in (BASIS_X, BASIS, BASIS.T, BASIS_X.T)])


def last_edge():
    wide = np.zeros((2, NG, 128))
    wide[0, :, :NG] = BASIS.T
    wide[1, :, 64 : 64 + NG] = BASIS.T
    return halves(wide)


LAST_HIGH, LAST_LOW = last_edge()


def split(x):
    high = x.astype(bf16)
    return high, (x - high.astype(f32)).astype(bf16)


def dot(a, b):
    return jnp.dot(a, b, preferred_element_type=f32)


def dot_t(a, b):
    return lax.dot_general(a, b, (((1,), (1,)), ((), ())), preferred_element_type=f32)


def left_mul(matrix, x):
    high, low = split(x)
    return dot(matrix, jnp.concatenate([high, low, high], 0))


def tables_kernel(high_ref, low_ref, wide_high, wide_low, coulomb):
    wide_high[...] = jnp.zeros_like(wide_high)
    wide_low[...] = jnp.zeros_like(wide_low)
    for w in range(2):
        for d in range(2):
            for i in range(4):
                rows = slice(48 * i + 64 * w, 48 * i + 64 * w + 48)
                cols = slice(128 * i, 128 * i + 128)
                wide_high[w, d, rows, cols] = high_ref[d]
                wide_low[w, d, rows, cols] = low_ref[d]

    def square(i):
        freq = jnp.where(i <= NG // 2, i, i - NG // 2).astype(f32)
        return freq * freq

    middle = lax.broadcasted_iota(jnp.int32, (NG, 128), 0)
    lane = lax.broadcasted_iota(jnp.int32, (NG, 128), 1)
    last = jnp.minimum(jnp.where(lane >= 64, lane - 64, lane), NG - 1)
    rest = square(middle) + square(last)
    for k in range(NG):
        total = rest + float(SQUARES[k])
        coulomb[k] = jnp.where(total > 0.0, -COULOMB / jnp.maximum(total, 1.0), 0.0)


def tables():
    wide = jax.ShapeDtypeStruct((2, 2, 256, 512), bf16)
    return pl.pallas_call(
        tables_kernel,
        out_shape=(wide, wide, jax.ShapeDtypeStruct((NG, NG, 128), f32)),
        name="tables",
    )(jnp.asarray(LAST_HIGH), jnp.asarray(LAST_LOW))


def exchange_kernel(
    own_ref, pair_ref, left_ref, wide_high, wide_low, coulomb, out_ref, rho_h, rho_l, za, zb, sol_h, sol_l
):
    def column(ref, first, c):
        return jnp.concatenate(
            [ref[pl.ds(first + COLS * p + c, SLABS, stride=ROWS), :] for p in range(PLANES)], 0
        )

    def place(c):
        return slice(48 * (c // 3), 48 * (c // 3) + 48), slice(128 * (c % 3), 128 * (c % 3) + 128)

    for c in range(COLS):
        own = column(own_ref, 0, c)
        rows, cols = place(c)
        for d in range(2):
            high, low = split(own * column(pair_ref, d * SLABS * ROWS, c))
            rho_h[d, rows, cols] = high
            rho_l[d, rows, cols] = low
    for w in range(2):
        window = slice(128 * w, 128 * w + 256)
        out = None
        for d in range(2):
            high, low = rho_h[d, :, window], rho_l[d, :, window]
            term = dot(high, wide_high[w, d]) + dot(low, wide_high[w, d]) + dot(high, wide_low[w, d])
            out = term if out is None else out + term
        for c in range(6):
            for i in range(4):
                y = 8 * c + 4 * w + i
                za[48 * y : 48 * y + 48, :] = out[48 * c : 48 * c + 48, 128 * i : 128 * i + 128]
    for y in range(0, NG, 2):
        both = jnp.concatenate([za[48 * y : 48 * y + 48, :], za[48 * y + 48 : 48 * y + 96, :]], 1)
        both = left_mul(left_ref[0], both)
        zb[48 * y : 48 * y + 48, :] = both[:, :128]
        zb[48 * y + 48 : 48 * y + 96, :] = both[:, 128:]
    for k in range(0, NG, 2):
        both = jnp.concatenate([zb[pl.ds(k, 48, stride=48), :], zb[pl.ds(k + 1, 48, stride=48), :]], 1)
        both = left_mul(left_ref[1], both) * jnp.concatenate([coulomb[k], coulomb[k + 1]], 1)
        both = left_mul(left_ref[2], both)
        za[pl.ds(k, 48, stride=48), :] = both[:, :128]
        za[pl.ds(k + 1, 48, stride=48), :] = both[:, 128:]
    for y in range(0, NG, 2):
        both = jnp.concatenate([za[48 * y : 48 * y + 48, :], za[48 * y + 48 : 48 * y + 96, :]], 1)
        both = left_mul(left_ref[3], both)
        for e in range(2):
            c, w, i = (y + e) // 8, ((y + e) % 8) // 4, (y + e) % 4
            high, low = split(both[:, 128 * e : 128 * e + 128])
            sol_h[w, 48 * c : 48 * c + 48, 128 * i : 128 * i + 128] = high
            sol_l[w, 48 * c : 48 * c + 48, 128 * i : 128 * i + 128] = low
    thirds = []
    for d in range(2):
        a, b = [
            dot_t(sol_h[w], wide_high[w, d]) + dot_t(sol_l[w], wide_high[w, d]) + dot_t(sol_h[w], wide_low[w, d])
            for w in range(2)
        ]
        thirds.append((a[:, :128], a[:, 128:] + b[:, :128], b[:, 128:]))
    for c in range(COLS):
        rows, _ = place(c)
        out = thirds[0][c % 3][rows] * column(pair_ref, 0, c)
        out = out + thirds[1][c % 3][rows] * column(pair_ref, SLABS * ROWS, c)
        for p in range(PLANES):
            out_ref[pl.ds(COLS * p + c, SLABS, stride=ROWS), :] = out[16 * p : 16 * p + 16]
    for r in range(USED, ROWS):
        out_ref[pl.ds(r, SLABS, stride=ROWS), :] = jnp.zeros((SLABS, 128), f32)


def partial_exchange(own, pair, made):
    big = pltpu.VMEM((NG * NG, 128), f32)
    rho, solved = pltpu.VMEM((2, 288, 384), bf16), pltpu.VMEM((2, 288, 512), bf16)
    return pl.pallas_call(
        exchange_kernel,
        out_shape=jax.ShapeDtypeStruct((SLABS * ROWS, 128), f32),
        scratch_shapes=[rho, rho, big, big, solved, solved],
        name="exchange",
    )(own, pair, jnp.asarray(LEFTS), *made)


def prepare_kernel(slab_ref, tile_ref, copies_ref):
    tile_ref[USED:ROWS, :] = jnp.zeros((ROWS - USED, 128), f32)
    for p in range(PLANES):
        for c in range(COLS):
            r = COLS * p + c
            tile_ref[r : r + 1, :] = slab_ref[p, :, 128 * c : 128 * c + 128]
    tile = tile_ref[...]
    for k in range(SLABS):
        copies_ref[k] = tile


def prepare(slab):
    tile = jax.ShapeDtypeStruct((ROWS, 128), f32)
    copies = jax.ShapeDtypeStruct((SLABS, ROWS, 128), f32)
    return pl.pallas_call(prepare_kernel, out_shape=(tile, copies), name="prepare")(slab)


def column_kernel(share_ref, orbital_ref, field_ref, copies_ref):
    field = jnp.sum(share_ref[...], axis=0)
    field_ref[...] = field
    sums = [
        jnp.sum(field * orbital_ref[ROWS * k : ROWS * k + ROWS, :], axis=0, keepdims=True) for k in range(BANDS)
    ]
    high, low = split(jnp.concatenate(sums + [jnp.zeros((128 - BANDS, 128), f32)], 0))
    ones = jnp.ones((8, 128), bf16)
    line = dot_t(ones, high) + dot_t(ones, low)
    for k in range(SLABS):
        copies_ref[k] = line


def column_part(shares, orbitals):
    field = jax.ShapeDtypeStruct((ROWS, 128), f32)
    copies = jax.ShapeDtypeStruct((SLABS, 8, 128), f32)
    return pl.pallas_call(column_kernel, out_shape=(field, copies), name="column")(shares, orbitals)


def attach_kernel(field_ref, parts_ref, copies_ref):
    column = jnp.sum(parts_ref[...], axis=0)[:1]
    row = lax.broadcasted_iota(jnp.int32, (ROWS, 128), 0)
    tile = jnp.where(row == USED, column, field_ref[...])
    for k in range(CHIPS):
        copies_ref[k] = tile


def attach(field, parts):
    copies = jax.ShapeDtypeStruct((CHIPS, ROWS, 128), f32)
    return pl.pallas_call(attach_kernel, out_shape=copies, name="attach")(field, parts)


BLOCK = 4


def place_of(band):
    return (band % 2) * CHIPS + band // 2


def finish_kernel(band_ref, field_ref, out_ref, flat):
    band = band_ref[0]
    matrix = field_ref[pl.ds(USED, BANDS, stride=ROWS), :][:, :BANDS]
    definite = (matrix + matrix.T) * (-0.5 / float(NG**3))
    row = lax.broadcasted_iota(jnp.int32, (BANDS, 2 * BANDS), 0)
    lane = lax.broadcasted_iota(jnp.int32, (BANDS, 2 * BANDS), 1)
    order = 2 * (row % CHIPS) + row // CHIPS
    unit = jnp.where(row[:, :BANDS] == lane[:, :BANDS], 1.0, 0.0).astype(f32)
    state = jnp.concatenate([definite, unit], 1)
    for first in range(0, BANDS, BLOCK):
        at = [place_of(first + i) for i in range(BLOCK)]
        columns = [jnp.broadcast_to(state[:, a : a + 1], (BANDS, 2 * BANDS)) for a in at]
        pivots = [state[a : a + 1, :] for a in at]
        for i in range(BLOCK):
            factor = jnp.where(order > first + i, columns[i] / columns[i][at[i] : at[i] + 1, :], 0.0)
            for j in range(i + 1, BLOCK):
                columns[j] = columns[j] - factor * columns[j][at[i] : at[i] + 1, :]
                pivots[j] = pivots[j] - factor[at[j] : at[j] + 1, :] * pivots[i]
            state = state - factor * pivots[i]
    mine = (band % 2) * CHIPS + band // 2
    picked = jnp.sum(jnp.where(row == mine, state, 0.0), axis=0, keepdims=True)
    pivot = jnp.sum(jnp.where(lane[:1] == mine, picked, 0.0), axis=1, keepdims=True)
    weights = picked * lax.rsqrt(pivot)
    total = None
    for k in range(BANDS):
        weight = weights[:, BANDS + k : BANDS + k + 1]
        term = weight * field_ref[ROWS * k : ROWS * k + ROWS, :]
        total = term if total is None else total + term
    flat[...] = total
    for p in range(PLANES):
        for c in range(COLS):
            r = COLS * p + c
            out_ref[p, :, 128 * c : 128 * c + 128] = flat[r : r + 1, :]


def finish(band, fields):
    return pl.pallas_call(
        finish_kernel,
        out_shape=jax.ShapeDtypeStruct((PLANES, 1, NG * NG), f32),
        in_specs=[pl.BlockSpec(memory_space=pltpu.SMEM), pl.BlockSpec(memory_space=pltpu.VMEM)],
        scratch_shapes=[pltpu.VMEM((ROWS, 128), f32)],
        name="finish",
    )(band, fields)


def exchange_tiles(tiles, axis):
    return lax.all_to_all(tiles, axis, 0, 0, tiled=True)


def both_cores(chips):
    return lax.all_gather(chips, "c", axis=0, tiled=False).reshape(BANDS * ROWS, 128)


def per_device(orbitals):
    tile, copies = prepare(jnp.transpose(orbitals, (1, 0, 2)))
    made = tables()
    moves = [
        (b * SLABS + s, (2 * s + b % 2) * SLABS + b // 2) for b in range(BANDS) for s in range(SLABS)
    ]
    partner = lax.ppermute(tile, BAND + GRID, moves)
    own = exchange_tiles(copies, GRID)
    own, partner = lax.optimization_barrier((own, partner))
    pair = exchange_tiles(jnp.broadcast_to(partner[None], copies.shape), PAIR)
    pair, copies = lax.optimization_barrier((pair, copies))
    slab_orbitals = exchange_tiles(copies, PAIR)
    partial = partial_exchange(own.reshape(SLABS * ROWS, 128), both_cores(pair), made)
    partial, slab_orbitals = lax.optimization_barrier((partial, slab_orbitals))
    shares = exchange_tiles(partial.reshape(SLABS, ROWS, 128), GRID)
    field, lines = column_part(shares, both_cores(slab_orbitals))
    parts = exchange_tiles(lines, GRID)
    fields = both_cores(exchange_tiles(attach(field, parts), PAIR))
    band = lax.axis_index(BAND).astype(jnp.int32).reshape(1)
    return jnp.transpose(finish(band, fields), (1, 0, 2))


def solution(mesh):
    parted = Mesh(mesh.devices.reshape(2, 8, 2, 2, 8), BAND + GRID)
    spec = P(BAND, GRID, None)
    return jax.shard_map(per_device, mesh=parted, in_specs=(spec,), out_specs=spec, check_vma=False)
```

```python
import math

import jax
import jax.numpy as jnp
import numpy as np
from jax import lax
from jax.experimental import pallas as pl
from jax.experimental.pallas import tpu as pltpu
from jax.sharding import Mesh, PartitionSpec as P

NG = 48
BANDS = 32
COULOMB = 50.0
SLABS = 16
PLANES = NG // SLABS
COLS = NG * NG // 128
ROWS = 56
USED = PLANES * COLS
CHIPS = BANDS // 2
PAIR, CORE, GRID = ("xl", "z4", "z2", "z1"), ("c",), ("xh", "y4", "y2", "y1")
BAND = PAIR + CORE
f32, bf16 = jnp.float32, jnp.bfloat16
SMALL = pltpu.CompilerParams(vmem_limit_bytes=12 << 20)
LARGE = pltpu.CompilerParams(vmem_limit_bytes=24 << 20)


def real_basis():
    half = NG // 2
    freq = np.concatenate([np.arange(half + 1), np.arange(1, half)])
    turn = 2.0 * np.pi * ((freq[:, None] * np.arange(NG)[None, :]) % NG) / NG
    wave = np.where(np.arange(NG)[:, None] <= half, np.cos(turn), np.sin(turn))
    norm = np.where((np.arange(NG) == 0) | (np.arange(NG) == half), 1.0, 2.0) / NG
    return wave * np.sqrt(norm)[:, None], freq.astype(np.float64) ** 2


def halves(matrix):
    high = matrix.astype(np.float32).astype(bf16)
    low = (matrix - high.astype(np.float64)).astype(np.float32).astype(bf16)
    return high, low


def from_left(matrix):
    high, low = halves(matrix)
    return np.concatenate([high, high, low], 1)


BASIS, SQUARES = real_basis()
BASIS_X = BASIS[:, [PLANES * (r % SLABS) + r // SLABS for r in range(NG)]]
LEFTS = np.stack([from_left(m) for m in (BASIS_X, BASIS, BASIS.T, BASIS_X.T)])


def last_edge():
    wide = np.zeros((2, NG, 128))
    wide[0, :, :NG] = BASIS.T
    wide[1, :, 64 : 64 + NG] = BASIS.T
    return halves(wide)


LAST_HIGH, LAST_LOW = last_edge()


def split(x):
    high = x.astype(bf16)
    return high, (x - high.astype(f32)).astype(bf16)


def dot(a, b):
    return jnp.dot(a, b, preferred_element_type=f32)


def dot_t(a, b):
    return lax.dot_general(a, b, (((1,), (1,)), ((), ())), preferred_element_type=f32)


def left_mul(matrix, x):
    high, low = split(x)
    return dot(matrix, jnp.concatenate([high, low, high], 0))


def tables_kernel(high_ref, low_ref, wide_high, wide_low, coulomb):
    wide_high[...] = jnp.zeros_like(wide_high)
    wide_low[...] = jnp.zeros_like(wide_low)
    for w in range(2):
        for d in range(2):
            for i in range(4):
                rows = slice(48 * i + 64 * w, 48 * i + 64 * w + 48)
                cols = slice(128 * i, 128 * i + 128)
                wide_high[w, d, rows, cols] = high_ref[d]
                wide_low[w, d, rows, cols] = low_ref[d]

    def square(i):
        freq = jnp.where(i <= NG // 2, i, i - NG // 2).astype(f32)
        return freq * freq

    middle = lax.broadcasted_iota(jnp.int32, (NG, 128), 0)
    lane = lax.broadcasted_iota(jnp.int32, (NG, 128), 1)
    last = jnp.minimum(jnp.where(lane >= 64, lane - 64, lane), NG - 1)
    rest = square(middle) + square(last)
    for k in range(NG):
        total = rest + float(SQUARES[k])
        coulomb[k] = jnp.where(total > 0.0, -COULOMB / jnp.maximum(total, 1.0), 0.0)


def tables():
    wide = jax.ShapeDtypeStruct((2, 2, 256, 512), bf16)
    return pl.pallas_call(
        tables_kernel,
        out_shape=(wide, wide, jax.ShapeDtypeStruct((NG, NG, 128), f32)),
        name="tables",
        compiler_params=SMALL,
    )(jnp.asarray(LAST_HIGH), jnp.asarray(LAST_LOW))


def exchange_kernel(
    own_ref, pair_ref, left_ref, wide_high, wide_low, coulomb, out_ref, rho_h, rho_l, za, zb, sol_h, sol_l
):
    def column(ref, first, c):
        return jnp.concatenate(
            [ref[pl.ds(first + COLS * p + c, SLABS, stride=ROWS), :] for p in range(PLANES)], 0
        )

    def partner(d, c):
        return column(pair_ref, d * SLABS * ROWS, c)

    def place(c):
        return slice(48 * (c // 3), 48 * (c // 3) + 48), slice(128 * (c % 3), 128 * (c % 3) + 128)

    for c in range(COLS):
        own = column(own_ref, 0, c)
        rows, cols = place(c)
        for d in range(2):
            high, low = split(own * partner(d, c))
            rho_h[d, rows, cols] = high
            rho_l[d, rows, cols] = low
    for w in range(2):
        window = slice(128 * w, 128 * w + 256)
        out = None
        for d in range(2):
            high, low = rho_h[d, :, window], rho_l[d, :, window]
            term = dot(high, wide_high[w, d]) + dot(low, wide_high[w, d]) + dot(high, wide_low[w, d])
            out = term if out is None else out + term
        for c in range(6):
            for i in range(4):
                y = 8 * c + 4 * w + i
                za[48 * y : 48 * y + 48, :] = out[48 * c : 48 * c + 48, 128 * i : 128 * i + 128]
    for y in range(0, NG, 2):
        both = jnp.concatenate([za[48 * y : 48 * y + 48, :], za[48 * y + 48 : 48 * y + 96, :]], 1)
        both = left_mul(left_ref[0], both)
        zb[48 * y : 48 * y + 48, :] = both[:, :128]
        zb[48 * y + 48 : 48 * y + 96, :] = both[:, 128:]
    for k in range(0, NG, 2):
        both = jnp.concatenate([zb[pl.ds(k, 48, stride=48), :], zb[pl.ds(k + 1, 48, stride=48), :]], 1)
        both = left_mul(left_ref[1], both) * jnp.concatenate([coulomb[k], coulomb[k + 1]], 1)
        both = left_mul(left_ref[2], both)
        za[pl.ds(k, 48, stride=48), :] = both[:, :128]
        za[pl.ds(k + 1, 48, stride=48), :] = both[:, 128:]
    for y in range(0, NG, 2):
        both = jnp.concatenate([za[48 * y : 48 * y + 48, :], za[48 * y + 48 : 48 * y + 96, :]], 1)
        both = left_mul(left_ref[3], both)
        for e in range(2):
            c, w, i = (y + e) // 8, ((y + e) % 8) // 4, (y + e) % 4
            high, low = split(both[:, 128 * e : 128 * e + 128])
            sol_h[w, 48 * c : 48 * c + 48, 128 * i : 128 * i + 128] = high
            sol_l[w, 48 * c : 48 * c + 48, 128 * i : 128 * i + 128] = low
    thirds = []
    for d in range(2):
        a, b = [
            dot_t(sol_h[w], wide_high[w, d]) + dot_t(sol_l[w], wide_high[w, d]) + dot_t(sol_h[w], wide_low[w, d])
            for w in range(2)
        ]
        thirds.append((a[:, :128], a[:, 128:] + b[:, :128], b[:, 128:]))
    for c in range(COLS):
        rows, _ = place(c)
        out = thirds[0][c % 3][rows] * partner(0, c)
        out = out + thirds[1][c % 3][rows] * partner(1, c)
        for p in range(PLANES):
            out_ref[pl.ds(COLS * p + c, SLABS, stride=ROWS), :] = out[16 * p : 16 * p + 16]
    for r in range(USED, ROWS):
        out_ref[pl.ds(r, SLABS, stride=ROWS), :] = jnp.zeros((SLABS, 128), f32)


def partial_exchange(own, pair, made):
    big = pltpu.VMEM((NG * NG, 128), f32)
    rho, solved = pltpu.VMEM((2, 288, 384), bf16), pltpu.VMEM((2, 288, 512), bf16)
    return pl.pallas_call(
        exchange_kernel,
        out_shape=jax.ShapeDtypeStruct((SLABS * ROWS, 128), f32),
        scratch_shapes=[rho, rho, big, big, solved, solved],
        name="exchange",
        compiler_params=LARGE,
    )(own, pair, jnp.asarray(LEFTS), *made)


def prepare_kernel(slab_ref, tile_ref, copies_ref):
    tile_ref[USED:ROWS, :] = jnp.zeros((ROWS - USED, 128), f32)
    for p in range(PLANES):
        for c in range(COLS):
            r = COLS * p + c
            tile_ref[r : r + 1, :] = slab_ref[p, :, 128 * c : 128 * c + 128]
    tile = tile_ref[...]
    for k in range(SLABS):
        copies_ref[k] = tile


def prepare(slab):
    tile = jax.ShapeDtypeStruct((ROWS, 128), f32)
    copies = jax.ShapeDtypeStruct((SLABS, ROWS, 128), f32)
    return pl.pallas_call(prepare_kernel, out_shape=(tile, copies), name="prepare", compiler_params=SMALL)(slab)


def column_kernel(share_ref, orbital_ref, line_ref, copies_ref):
    field = jnp.sum(share_ref[...], axis=0)
    for k in range(CHIPS):
        copies_ref[k] = field
    sums = [
        jnp.sum(field * orbital_ref[ROWS * k : ROWS * k + ROWS, :], axis=0, keepdims=True) for k in range(BANDS)
    ]
    high, low = split(jnp.concatenate(sums + [jnp.zeros((128 - BANDS, 128), f32)], 0))
    ones = jnp.ones((8, 128), bf16)
    line_ref[...] = (dot_t(ones, high) + dot_t(ones, low))[:1]


def column_part(shares, orbitals):
    line = jax.ShapeDtypeStruct((1, 128), f32)
    copies = jax.ShapeDtypeStruct((CHIPS, ROWS, 128), f32)
    return pl.pallas_call(
        column_kernel, out_shape=(line, copies), name="column", compiler_params=SMALL
    )(shares, orbitals)


def pack_kernel(column_ref, copies_ref):
    packed = jnp.concatenate([column_ref[8 * q : 8 * q + 8, :BANDS] for q in range(4)], 1)
    for k in range(SLABS):
        copies_ref[k] = packed


def pack(columns):
    copies = jax.ShapeDtypeStruct((SLABS, 8, 128), f32)
    return pl.pallas_call(pack_kernel, out_shape=copies, name="pack", compiler_params=SMALL)(columns)


BLOCK = 4


def place_of(band):
    return (band % 2) * CHIPS + band // 2


def finish_kernel(band_ref, part_ref, field_ref, out_ref, flat):
    band = band_ref[0]
    packed = jnp.sum(part_ref[...], axis=0)
    matrix = jnp.concatenate([packed[:, 32 * q : 32 * q + 32] for q in range(4)], 0)
    definite = (matrix + matrix.T) * (-0.5 / float(NG**3))
    row = lax.broadcasted_iota(jnp.int32, (BANDS, 2 * BANDS), 0)
    lane = lax.broadcasted_iota(jnp.int32, (BANDS, 2 * BANDS), 1)
    order = 2 * (row % CHIPS) + row // CHIPS
    unit = jnp.where(row[:, :BANDS] == lane[:, :BANDS], 1.0, 0.0).astype(f32)
    state = jnp.concatenate([definite, unit], 1)
    for first in range(0, BANDS, BLOCK):
        at = [place_of(first + i) for i in range(BLOCK)]
        columns = [jnp.broadcast_to(state[:, a : a + 1], (BANDS, 2 * BANDS)) for a in at]
        pivots = [state[a : a + 1, :] for a in at]
        for i in range(BLOCK):
            factor = jnp.where(order > first + i, columns[i] / columns[i][at[i] : at[i] + 1, :], 0.0)
            for j in range(i + 1, BLOCK):
                columns[j] = columns[j] - factor * columns[j][at[i] : at[i] + 1, :]
                pivots[j] = pivots[j] - factor[at[j] : at[j] + 1, :] * pivots[i]
            state = state - factor * pivots[i]
    mine = (band % 2) * CHIPS + band // 2
    picked = jnp.sum(jnp.where(row == mine, state, 0.0), axis=0, keepdims=True)
    pivot = jnp.sum(jnp.where(lane[:1] == mine, picked, 0.0), axis=1, keepdims=True)
    weights = picked * lax.rsqrt(pivot)
    total = None
    for k in range(BANDS):
        weight = weights[:, BANDS + k : BANDS + k + 1]
        term = weight * field_ref[ROWS * k : ROWS * k + ROWS, :]
        total = term if total is None else total + term
    flat[...] = total
    for p in range(PLANES):
        for c in range(COLS):
            r = COLS * p + c
            out_ref[p, :, 128 * c : 128 * c + 128] = flat[r : r + 1, :]


def finish(band, parts, fields):
    vmem = pl.BlockSpec(memory_space=pltpu.VMEM)
    return pl.pallas_call(
        finish_kernel,
        out_shape=jax.ShapeDtypeStruct((PLANES, 1, NG * NG), f32),
        in_specs=[pl.BlockSpec(memory_space=pltpu.SMEM), vmem, vmem],
        scratch_shapes=[pltpu.VMEM((ROWS, 128), f32)],
        name="finish",
        compiler_params=SMALL,
    )(band, parts, fields)


def exchange_tiles(tiles, axis):
    return lax.all_to_all(tiles, axis, 0, 0, tiled=True)


def both_cores(chips):
    return lax.all_gather(chips, CORE, axis=0, tiled=False).reshape(-1, 128)


def per_device(orbitals):
    tile, copies = prepare(jnp.transpose(orbitals, (1, 0, 2)))
    made = tables()
    moves = [
        (b * SLABS + s, (2 * s + b % 2) * SLABS + b // 2) for b in range(BANDS) for s in range(SLABS)
    ]
    partner = lax.ppermute(tile, BAND + GRID, moves)
    own = exchange_tiles(copies, GRID)
    own, partner, *made = lax.optimization_barrier((own, partner, *made))
    both = jnp.concatenate([partner, tile], 0)
    both = exchange_tiles(jnp.broadcast_to(both[None], (CHIPS, 2 * ROWS, 128)), PAIR)
    pair = both_cores(both[:, :ROWS])
    partial = partial_exchange(own.reshape(SLABS * ROWS, 128), pair, made)
    partial, others = lax.optimization_barrier((partial, both[:, ROWS:]))
    shares = exchange_tiles(partial.reshape(SLABS, ROWS, 128), GRID)
    columns, copies = column_part(shares, both_cores(others))
    fields = exchange_tiles(copies, PAIR)
    for axes in (("z2", "z1"), "z4", "xl", "c"):
        columns = lax.all_gather(columns, axes, axis=0, tiled=True)
    parts = pack(columns)
    parts, fields = lax.optimization_barrier((parts, fields))
    parts = exchange_tiles(parts, GRID)
    band = lax.axis_index(BAND).astype(jnp.int32).reshape(1)
    return jnp.transpose(finish(band, parts, both_cores(fields)), (1, 0, 2))


def solution(mesh):
    parted = Mesh(mesh.devices.reshape((2,) * 9), BAND + GRID)
    spec = P(BAND, GRID, None)
    return jax.shard_map(per_device, mesh=parted, in_specs=(spec,), out_specs=spec, check_vma=False)
```

```python
import math

import jax
import jax.numpy as jnp
import numpy as np
from jax import lax
from jax.experimental import pallas as pl
from jax.experimental.pallas import tpu as pltpu
from jax.sharding import Mesh, PartitionSpec as P

NG = 48
BANDS = 32
COULOMB = 50.0
SLABS = 16
PLANES = NG // SLABS
COLS = NG * NG // 128
ROWS = 56
USED = PLANES * COLS
CHIPS = BANDS // 2
PAIR, CORE, GRID = ("xl", "z4", "z2", "z1"), ("c",), ("xh", "y4", "y2", "y1")
BAND = PAIR + CORE
f32, bf16 = jnp.float32, jnp.bfloat16
SMALL = pltpu.CompilerParams(vmem_limit_bytes=12 << 20)
LARGE = pltpu.CompilerParams(vmem_limit_bytes=24 << 20)


def real_basis():
    half = NG // 2
    freq = np.concatenate([np.arange(half + 1), np.arange(1, half)])
    turn = 2.0 * np.pi * ((freq[:, None] * np.arange(NG)[None, :]) % NG) / NG
    wave = np.where(np.arange(NG)[:, None] <= half, np.cos(turn), np.sin(turn))
    norm = np.where((np.arange(NG) == 0) | (np.arange(NG) == half), 1.0, 2.0) / NG
    return wave * np.sqrt(norm)[:, None], freq.astype(np.float64) ** 2


def halves(matrix):
    high = matrix.astype(np.float32).astype(bf16)
    low = (matrix - high.astype(np.float64)).astype(np.float32).astype(bf16)
    return high, low


def from_left(matrix):
    high, low = halves(matrix)
    return np.concatenate([high, high, low], 1)


BASIS, SQUARES = real_basis()
BASIS_X = BASIS[:, [PLANES * (r % SLABS) + r // SLABS for r in range(NG)]]
LEFTS = np.stack([from_left(m) for m in (BASIS_X, BASIS, BASIS.T, BASIS_X.T)])


def last_edge():
    wide = np.zeros((2, NG, 128))
    wide[0, :, :NG] = BASIS.T
    wide[1, :, 64 : 64 + NG] = BASIS.T
    return halves(wide)


LAST_HIGH, LAST_LOW = last_edge()


def split(x):
    high = x.astype(bf16)
    return high, (x - high.astype(f32)).astype(bf16)


def dot(a, b):
    return jnp.dot(a, b, preferred_element_type=f32)


def dot_t(a, b):
    return lax.dot_general(a, b, (((1,), (1,)), ((), ())), preferred_element_type=f32)


def left_mul(matrix, x):
    high, low = split(x)
    return dot(matrix, jnp.concatenate([high, low, high], 0))


def tables_kernel(high_ref, low_ref, wide_high, wide_low, coulomb):
    wide_high[...] = jnp.zeros_like(wide_high)
    wide_low[...] = jnp.zeros_like(wide_low)
    for w in range(2):
        for d in range(2):
            for i in range(4):
                rows = slice(48 * i + 64 * w, 48 * i + 64 * w + 48)
                cols = slice(128 * i, 128 * i + 128)
                wide_high[w, d, rows, cols] = high_ref[d]
                wide_low[w, d, rows, cols] = low_ref[d]

    def square(i):
        freq = jnp.where(i <= NG // 2, i, i - NG // 2).astype(f32)
        return freq * freq

    middle = lax.broadcasted_iota(jnp.int32, (NG, 128), 0)
    lane = lax.broadcasted_iota(jnp.int32, (NG, 128), 1)
    last = jnp.minimum(jnp.where(lane >= 64, lane - 64, lane), NG - 1)
    rest = square(middle) + square(last)
    for k in range(NG):
        total = rest + float(SQUARES[k])
        coulomb[k] = jnp.where(total > 0.0, -COULOMB / jnp.maximum(total, 1.0), 0.0)


def tables():
    wide = jax.ShapeDtypeStruct((2, 2, 256, 512), bf16)
    return pl.pallas_call(
        tables_kernel,
        out_shape=(wide, wide, jax.ShapeDtypeStruct((NG, NG, 128), f32)),
        name="tables",
        compiler_params=SMALL,
    )(jnp.asarray(LAST_HIGH), jnp.asarray(LAST_LOW))


def exchange_kernel(
    own_ref, pair_ref, left_ref, wide_high, wide_low, coulomb, out_ref, rho_h, rho_l, za, zb, sol_h, sol_l
):
    def column(ref, first, c):
        return jnp.concatenate(
            [ref[pl.ds(first + COLS * p + c, SLABS, stride=ROWS), :] for p in range(PLANES)], 0
        )

    def partner(d, c):
        return column(pair_ref, d * SLABS * ROWS, c)

    def place(c):
        return slice(48 * (c // 3), 48 * (c // 3) + 48), slice(128 * (c % 3), 128 * (c % 3) + 128)

    for c in range(COLS):
        own = column(own_ref, 0, c)
        rows, cols = place(c)
        for d in range(2):
            high, low = split(own * partner(d, c))
            rho_h[d, rows, cols] = high
            rho_l[d, rows, cols] = low
    for w in range(2):
        window = slice(128 * w, 128 * w + 256)
        out = None
        for d in range(2):
            high, low = rho_h[d, :, window], rho_l[d, :, window]
            term = dot(high, wide_high[w, d]) + dot(low, wide_high[w, d]) + dot(high, wide_low[w, d])
            out = term if out is None else out + term
        for c in range(6):
            for i in range(4):
                y = 8 * c + 4 * w + i
                za[48 * y : 48 * y + 48, :] = out[48 * c : 48 * c + 48, 128 * i : 128 * i + 128]
    for y in range(0, NG, 2):
        both = jnp.concatenate([za[48 * y : 48 * y + 48, :], za[48 * y + 48 : 48 * y + 96, :]], 1)
        both = left_mul(left_ref[0], both)
        zb[48 * y : 48 * y + 48, :] = both[:, :128]
        zb[48 * y + 48 : 48 * y + 96, :] = both[:, 128:]
    for k in range(0, NG, 2):
        both = jnp.concatenate([zb[pl.ds(k, 48, stride=48), :], zb[pl.ds(k + 1, 48, stride=48), :]], 1)
        both = left_mul(left_ref[1], both) * jnp.concatenate([coulomb[k], coulomb[k + 1]], 1)
        both = left_mul(left_ref[2], both)
        za[pl.ds(k, 48, stride=48), :] = both[:, :128]
        za[pl.ds(k + 1, 48, stride=48), :] = both[:, 128:]
    for y in range(0, NG, 2):
        both = jnp.concatenate([za[48 * y : 48 * y + 48, :], za[48 * y + 48 : 48 * y + 96, :]], 1)
        both = left_mul(left_ref[3], both)
        for e in range(2):
            c, w, i = (y + e) // 8, ((y + e) % 8) // 4, (y + e) % 4
            high, low = split(both[:, 128 * e : 128 * e + 128])
            sol_h[w, 48 * c : 48 * c + 48, 128 * i : 128 * i + 128] = high
            sol_l[w, 48 * c : 48 * c + 48, 128 * i : 128 * i + 128] = low
    thirds = []
    for d in range(2):
        a, b = [
            dot_t(sol_h[w], wide_high[w, d]) + dot_t(sol_l[w], wide_high[w, d]) + dot_t(sol_h[w], wide_low[w, d])
            for w in range(2)
        ]
        thirds.append((a[:, :128], a[:, 128:] + b[:, :128], b[:, 128:]))
    for c in range(COLS):
        rows, _ = place(c)
        out = thirds[0][c % 3][rows] * partner(0, c)
        out = out + thirds[1][c % 3][rows] * partner(1, c)
        for p in range(PLANES):
            out_ref[pl.ds(COLS * p + c, SLABS, stride=ROWS), :] = out[16 * p : 16 * p + 16]
    for r in range(USED, ROWS):
        out_ref[pl.ds(r, SLABS, stride=ROWS), :] = jnp.zeros((SLABS, 128), f32)


def partial_exchange(own, pair, made):
    big = pltpu.VMEM((NG * NG, 128), f32)
    rho, solved = pltpu.VMEM((2, 288, 384), bf16), pltpu.VMEM((2, 288, 512), bf16)
    return pl.pallas_call(
        exchange_kernel,
        out_shape=jax.ShapeDtypeStruct((SLABS * ROWS, 128), f32),
        scratch_shapes=[rho, rho, big, big, solved, solved],
        name="exchange",
        compiler_params=LARGE,
    )(own, pair, jnp.asarray(LEFTS), *made)


def prepare_kernel(slab_ref, copies_ref, tile_ref):
    tile_ref[USED:ROWS, :] = jnp.zeros((ROWS - USED, 128), f32)
    for p in range(PLANES):
        for c in range(COLS):
            r = COLS * p + c
            tile_ref[r : r + 1, :] = slab_ref[p, :, 128 * c : 128 * c + 128]
    tile = tile_ref[...]
    for k in range(SLABS):
        copies_ref[k] = tile


def prepare(slab):
    return pl.pallas_call(
        prepare_kernel,
        out_shape=jax.ShapeDtypeStruct((SLABS, ROWS, 128), f32),
        scratch_shapes=[pltpu.VMEM((ROWS, 128), f32)],
        name="prepare",
        compiler_params=SMALL,
    )(slab)


def column_kernel(share_ref, orbital_ref, field_ref, copies_ref):
    field = jnp.sum(share_ref[...], axis=0)
    field_ref[...] = field
    sums = [
        jnp.sum(field * orbital_ref[ROWS * k : ROWS * k + ROWS, :], axis=0, keepdims=True) for k in range(BANDS)
    ]
    high, low = split(jnp.concatenate(sums + [jnp.zeros((128 - BANDS, 128), f32)], 0))
    ones = jnp.ones((8, 128), bf16)
    line = dot_t(ones, high) + dot_t(ones, low)
    for k in range(SLABS):
        copies_ref[k] = line


def column_part(shares, orbitals):
    field = jax.ShapeDtypeStruct((ROWS, 128), f32)
    copies = jax.ShapeDtypeStruct((SLABS, 8, 128), f32)
    return pl.pallas_call(column_kernel, out_shape=(field, copies), name="column", compiler_params=SMALL)(
        shares, orbitals
    )


def attach_kernel(field_ref, parts_ref, copies_ref):
    column = jnp.sum(parts_ref[...], axis=0)[:1]
    row = lax.broadcasted_iota(jnp.int32, (ROWS, 128), 0)
    tile = jnp.where(row == USED, column, field_ref[...])
    for k in range(CHIPS):
        copies_ref[k] = tile


def attach(field, parts):
    copies = jax.ShapeDtypeStruct((CHIPS, ROWS, 128), f32)
    return pl.pallas_call(attach_kernel, out_shape=copies, name="attach", compiler_params=SMALL)(field, parts)


BLOCK = 4


def place_of(band):
    return (band % 2) * CHIPS + band // 2


def finish_kernel(band_ref, field_ref, out_ref, flat):
    band = band_ref[0]
    matrix = field_ref[pl.ds(USED, BANDS, stride=ROWS), :][:, :BANDS]
    definite = (matrix + matrix.T) * (-0.5 / float(NG**3))
    row = lax.broadcasted_iota(jnp.int32, (BANDS, 2 * BANDS), 0)
    lane = lax.broadcasted_iota(jnp.int32, (BANDS, 2 * BANDS), 1)
    order = 2 * (row % CHIPS) + row // CHIPS
    unit = jnp.where(row[:, :BANDS] == lane[:, :BANDS], 1.0, 0.0).astype(f32)
    state = jnp.concatenate([definite, unit], 1)
    for first in range(0, BANDS, BLOCK):
        at = [place_of(first + i) for i in range(BLOCK)]
        columns = [jnp.broadcast_to(state[:, a : a + 1], (BANDS, 2 * BANDS)) for a in at]
        pivots = [state[a : a + 1, :] for a in at]
        for i in range(BLOCK):
            factor = jnp.where(order > first + i, columns[i] / columns[i][at[i] : at[i] + 1, :], 0.0)
            for j in range(i + 1, BLOCK):
                columns[j] = columns[j] - factor * columns[j][at[i] : at[i] + 1, :]
                pivots[j] = pivots[j] - factor[at[j] : at[j] + 1, :] * pivots[i]
            state = state - factor * pivots[i]
    mine = (band % 2) * CHIPS + band // 2
    picked = jnp.sum(jnp.where(row == mine, state, 0.0), axis=0, keepdims=True)
    pivot = jnp.sum(jnp.where(lane[:1] == mine, picked, 0.0), axis=1, keepdims=True)
    weights = picked * lax.rsqrt(pivot)
    total = None
    for k in range(BANDS):
        weight = weights[:, BANDS + k : BANDS + k + 1]
        term = weight * field_ref[ROWS * k : ROWS * k + ROWS, :]
        total = term if total is None else total + term
    flat[...] = total
    for p in range(PLANES):
        for c in range(COLS):
            r = COLS * p + c
            out_ref[p, :, 128 * c : 128 * c + 128] = flat[r : r + 1, :]


def finish(band, fields):
    return pl.pallas_call(
        finish_kernel,
        out_shape=jax.ShapeDtypeStruct((PLANES, 1, NG * NG), f32),
        in_specs=[pl.BlockSpec(memory_space=pltpu.SMEM), pl.BlockSpec(memory_space=pltpu.VMEM)],
        scratch_shapes=[pltpu.VMEM((ROWS, 128), f32)],
        name="finish",
        compiler_params=SMALL,
    )(band, fields)


def exchange_tiles(tiles, axis):
    return lax.all_to_all(tiles, axis, 0, 0, tiled=True)


def both_cores(chips):
    return lax.all_gather(chips, CORE, axis=0, tiled=False).reshape(-1, 128)


def per_device(orbitals):
    copies = prepare(jnp.transpose(orbitals, (1, 0, 2)))
    made = tables()
    chips = exchange_tiles(copies, PAIR)
    whole = exchange_tiles(jnp.concatenate([copies, chips], 1), GRID)
    pair = both_cores(whole[:, ROWS:])
    partial = partial_exchange(whole[:, :ROWS].reshape(SLABS * ROWS, 128), pair, made)
    shares = exchange_tiles(partial.reshape(SLABS, ROWS, 128), GRID)
    field, lines = column_part(shares, both_cores(chips))
    parts = exchange_tiles(lines, GRID)
    fields = both_cores(exchange_tiles(attach(field, parts), PAIR))
    band = lax.axis_index(BAND).astype(jnp.int32).reshape(1)
    return jnp.transpose(finish(band, fields), (1, 0, 2))


def solution(mesh):
    parted = Mesh(mesh.devices.reshape((2,) * 9), BAND + GRID)
    spec = P(BAND, GRID, None)
    return jax.shard_map(per_device, mesh=parted, in_specs=(spec,), out_specs=spec, check_vma=False)
```

```python
import math

import jax
import jax.numpy as jnp
import numpy as np
from jax import lax
from jax.experimental import pallas as pl
from jax.experimental.pallas import tpu as pltpu
from jax.sharding import Mesh, PartitionSpec as P

NG = 48
BANDS = 32
COULOMB = 50.0
SLABS = 16
PLANES = NG // SLABS
COLS = NG * NG // 128
ROWS = 56
USED = PLANES * COLS
CHIPS = BANDS // 2
PAIR, CORE, GRID = ("xl", "z4", "z2", "z1"), ("c",), ("xh", "y4", "y2", "y1")
BAND = PAIR + CORE
f32, bf16 = jnp.float32, jnp.bfloat16
SMALL = pltpu.CompilerParams(vmem_limit_bytes=12 << 20)
LARGE = pltpu.CompilerParams(vmem_limit_bytes=24 << 20)


def real_basis():
    half = NG // 2
    freq = np.concatenate([np.arange(half + 1), np.arange(1, half)])
    turn = 2.0 * np.pi * ((freq[:, None] * np.arange(NG)[None, :]) % NG) / NG
    wave = np.where(np.arange(NG)[:, None] <= half, np.cos(turn), np.sin(turn))
    norm = np.where((np.arange(NG) == 0) | (np.arange(NG) == half), 1.0, 2.0) / NG
    return wave * np.sqrt(norm)[:, None], freq.astype(np.float64) ** 2


def halves(matrix):
    high = matrix.astype(np.float32).astype(bf16)
    low = (matrix - high.astype(np.float64)).astype(np.float32).astype(bf16)
    return high, low


def from_left(matrix):
    high, low = halves(matrix)
    return np.concatenate([high, high, low], 1)


BASIS, SQUARES = real_basis()
BASIS_X = BASIS[:, [PLANES * (r % SLABS) + r // SLABS for r in range(NG)]]
LEFTS = np.stack([from_left(m) for m in (BASIS_X, BASIS, BASIS.T, BASIS_X.T)])


def last_edge():
    wide = np.zeros((2, NG, 128))
    wide[0, :, :NG] = BASIS.T
    wide[1, :, 64 : 64 + NG] = BASIS.T
    return halves(wide)


LAST_HIGH, LAST_LOW = last_edge()


def split(x):
    high = x.astype(bf16)
    return high, (x - high.astype(f32)).astype(bf16)


def dot(a, b):
    return jnp.dot(a, b, preferred_element_type=f32)


def dot_t(a, b):
    return lax.dot_general(a, b, (((1,), (1,)), ((), ())), preferred_element_type=f32)


def left_mul(matrix, x):
    high, low = split(x)
    return dot(matrix, jnp.concatenate([high, low, high], 0))


def tables_kernel(high_ref, low_ref, wide_high, wide_low, coulomb):
    wide_high[...] = jnp.zeros_like(wide_high)
    wide_low[...] = jnp.zeros_like(wide_low)
    for w in range(2):
        for d in range(2):
            for i in range(4):
                rows = slice(48 * i + 64 * w, 48 * i + 64 * w + 48)
                cols = slice(128 * i, 128 * i + 128)
                wide_high[w, d, rows, cols] = high_ref[d]
                wide_low[w, d, rows, cols] = low_ref[d]

    def square(i):
        freq = jnp.where(i <= NG // 2, i, i - NG // 2).astype(f32)
        return freq * freq

    middle = lax.broadcasted_iota(jnp.int32, (NG, 128), 0)
    lane = lax.broadcasted_iota(jnp.int32, (NG, 128), 1)
    last = jnp.minimum(jnp.where(lane >= 64, lane - 64, lane), NG - 1)
    rest = square(middle) + square(last)
    for k in range(NG):
        total = rest + float(SQUARES[k])
        coulomb[k] = jnp.where(total > 0.0, -COULOMB / jnp.maximum(total, 1.0), 0.0)


def tables(last_high, last_low):
    wide = jax.ShapeDtypeStruct((2, 2, 256, 512), bf16)
    return pl.pallas_call(
        tables_kernel,
        out_shape=(wide, wide, jax.ShapeDtypeStruct((NG, NG, 128), f32)),
        name="tables",
        compiler_params=SMALL,
    )(last_high, last_low)


def exchange_kernel(
    own_ref, pair_ref, left_ref, wide_high, wide_low, coulomb, out_ref, rho_h, rho_l, za, zb, sol_h, sol_l
):
    def column(ref, first, c):
        return jnp.concatenate(
            [ref[pl.ds(first + COLS * p + c, SLABS, stride=ROWS), :] for p in range(PLANES)], 0
        )

    def partner(d, c):
        return column(pair_ref, d * SLABS * ROWS, c)

    def place(c):
        return slice(48 * (c // 3), 48 * (c // 3) + 48), slice(128 * (c % 3), 128 * (c % 3) + 128)

    for c in range(COLS):
        own = column(own_ref, 0, c)
        rows, cols = place(c)
        for d in range(2):
            high, low = split(own * partner(d, c))
            rho_h[d, rows, cols] = high
            rho_l[d, rows, cols] = low
    for w in range(2):
        window = slice(128 * w, 128 * w + 256)
        out = None
        for d in range(2):
            high, low = rho_h[d, :, window], rho_l[d, :, window]
            term = dot(high, wide_high[w, d]) + dot(low, wide_high[w, d]) + dot(high, wide_low[w, d])
            out = term if out is None else out + term
        for c in range(6):
            for i in range(4):
                y = 8 * c + 4 * w + i
                za[48 * y : 48 * y + 48, :] = out[48 * c : 48 * c + 48, 128 * i : 128 * i + 128]
    for y in range(0, NG, 2):
        both = jnp.concatenate([za[48 * y : 48 * y + 48, :], za[48 * y + 48 : 48 * y + 96, :]], 1)
        both = left_mul(left_ref[0], both)
        zb[48 * y : 48 * y + 48, :] = both[:, :128]
        zb[48 * y + 48 : 48 * y + 96, :] = both[:, 128:]
    for k in range(0, NG, 2):
        both = jnp.concatenate([zb[pl.ds(k, 48, stride=48), :], zb[pl.ds(k + 1, 48, stride=48), :]], 1)
        both = left_mul(left_ref[1], both) * jnp.concatenate([coulomb[k], coulomb[k + 1]], 1)
        both = left_mul(left_ref[2], both)
        za[pl.ds(k, 48, stride=48), :] = both[:, :128]
        za[pl.ds(k + 1, 48, stride=48), :] = both[:, 128:]
    for y in range(0, NG, 2):
        both = jnp.concatenate([za[48 * y : 48 * y + 48, :], za[48 * y + 48 : 48 * y + 96, :]], 1)
        both = left_mul(left_ref[3], both)
        for e in range(2):
            c, w, i = (y + e) // 8, ((y + e) % 8) // 4, (y + e) % 4
            high, low = split(both[:, 128 * e : 128 * e + 128])
            sol_h[w, 48 * c : 48 * c + 48, 128 * i : 128 * i + 128] = high
            sol_l[w, 48 * c : 48 * c + 48, 128 * i : 128 * i + 128] = low
    thirds = []
    for d in range(2):
        a, b = [
            dot_t(sol_h[w], wide_high[w, d]) + dot_t(sol_l[w], wide_high[w, d]) + dot_t(sol_h[w], wide_low[w, d])
            for w in range(2)
        ]
        thirds.append((a[:, :128], a[:, 128:] + b[:, :128], b[:, 128:]))
    for c in range(COLS):
        rows, _ = place(c)
        out = thirds[0][c % 3][rows] * partner(0, c)
        out = out + thirds[1][c % 3][rows] * partner(1, c)
        for p in range(PLANES):
            out_ref[pl.ds(COLS * p + c, SLABS, stride=ROWS), :] = out[16 * p : 16 * p + 16]
    for r in range(USED, ROWS):
        out_ref[pl.ds(r, SLABS, stride=ROWS), :] = jnp.zeros((SLABS, 128), f32)


def partial_exchange(own, pair, made):
    big = pltpu.VMEM((NG * NG, 128), f32)
    rho, solved = pltpu.VMEM((2, 288, 384), bf16), pltpu.VMEM((2, 288, 512), bf16)
    return pl.pallas_call(
        exchange_kernel,
        out_shape=jax.ShapeDtypeStruct((SLABS * ROWS, 128), f32),
        scratch_shapes=[rho, rho, big, big, solved, solved],
        name="exchange",
        compiler_params=LARGE,
    )(own, pair, jnp.asarray(LEFTS), *made)


def prepare_kernel(slab_ref, tile_ref, copies_ref):
    tile_ref[USED:ROWS, :] = jnp.zeros((ROWS - USED, 128), f32)
    for p in range(PLANES):
        for c in range(COLS):
            r = COLS * p + c
            tile_ref[r : r + 1, :] = slab_ref[p, :, 128 * c : 128 * c + 128]
    tile = tile_ref[...]
    for k in range(SLABS):
        copies_ref[k] = tile


def prepare(slab):
    tile = jax.ShapeDtypeStruct((ROWS, 128), f32)
    copies = jax.ShapeDtypeStruct((SLABS, ROWS, 128), f32)
    return pl.pallas_call(prepare_kernel, out_shape=(tile, copies), name="prepare", compiler_params=SMALL)(slab)


def column_kernel(share_ref, orbital_ref, field_ref, copies_ref):
    field = jnp.sum(share_ref[...], axis=0)
    field_ref[...] = field
    sums = [
        jnp.sum(field * orbital_ref[ROWS * k : ROWS * k + ROWS, :], axis=0, keepdims=True) for k in range(BANDS)
    ]
    high, low = split(jnp.concatenate(sums + [jnp.zeros((128 - BANDS, 128), f32)], 0))
    ones = jnp.ones((8, 128), bf16)
    line = dot_t(ones, high) + dot_t(ones, low)
    for k in range(SLABS):
        copies_ref[k] = line


def column_part(shares, orbitals):
    field = jax.ShapeDtypeStruct((ROWS, 128), f32)
    copies = jax.ShapeDtypeStruct((SLABS, 8, 128), f32)
    return pl.pallas_call(column_kernel, out_shape=(field, copies), name="column", compiler_params=SMALL)(
        shares, orbitals
    )


def attach_kernel(field_ref, parts_ref, copies_ref):
    column = jnp.sum(parts_ref[...], axis=0)[:1]
    row = lax.broadcasted_iota(jnp.int32, (ROWS, 128), 0)
    tile = jnp.where(row == USED, column, field_ref[...])
    for k in range(CHIPS):
        copies_ref[k] = tile


def attach(field, parts):
    copies = jax.ShapeDtypeStruct((CHIPS, ROWS, 128), f32)
    return pl.pallas_call(attach_kernel, out_shape=copies, name="attach", compiler_params=SMALL)(field, parts)


BLOCK = 4


def place_of(band):
    return (band % 2) * CHIPS + band // 2


def finish_kernel(band_ref, field_ref, out_ref, flat):
    band = band_ref[0]
    matrix = field_ref[pl.ds(USED, BANDS, stride=ROWS), :][:, :BANDS]
    definite = (matrix + matrix.T) * (-0.5 / float(NG**3))
    row = lax.broadcasted_iota(jnp.int32, (BANDS, 2 * BANDS), 0)
    lane = lax.broadcasted_iota(jnp.int32, (BANDS, 2 * BANDS), 1)
    order = 2 * (row % CHIPS) + row // CHIPS
    unit = jnp.where(row[:, :BANDS] == lane[:, :BANDS], 1.0, 0.0).astype(f32)
    state = jnp.concatenate([definite, unit], 1)
    for first in range(0, BANDS, BLOCK):
        at = [place_of(first + i) for i in range(BLOCK)]
        columns = [jnp.broadcast_to(state[:, a : a + 1], (BANDS, 2 * BANDS)) for a in at]
        pivots = [state[a : a + 1, :] for a in at]
        for i in range(BLOCK):
            factor = jnp.where(order > first + i, columns[i] / columns[i][at[i] : at[i] + 1, :], 0.0)
            for j in range(i + 1, BLOCK):
                columns[j] = columns[j] - factor * columns[j][at[i] : at[i] + 1, :]
                pivots[j] = pivots[j] - factor[at[j] : at[j] + 1, :] * pivots[i]
            state = state - factor * pivots[i]
    mine = (band % 2) * CHIPS + band // 2
    picked = jnp.sum(jnp.where(row == mine, state, 0.0), axis=0, keepdims=True)
    pivot = jnp.sum(jnp.where(lane[:1] == mine, picked, 0.0), axis=1, keepdims=True)
    weights = picked * lax.rsqrt(pivot)
    total = None
    for k in range(BANDS):
        weight = weights[:, BANDS + k : BANDS + k + 1]
        term = weight * field_ref[ROWS * k : ROWS * k + ROWS, :]
        total = term if total is None else total + term
    flat[...] = total
    for p in range(PLANES):
        for c in range(COLS):
            r = COLS * p + c
            out_ref[p, :, 128 * c : 128 * c + 128] = flat[r : r + 1, :]


def finish(band, fields):
    return pl.pallas_call(
        finish_kernel,
        out_shape=jax.ShapeDtypeStruct((PLANES, 1, NG * NG), f32),
        in_specs=[pl.BlockSpec(memory_space=pltpu.SMEM), pl.BlockSpec(memory_space=pltpu.VMEM)],
        scratch_shapes=[pltpu.VMEM((ROWS, 128), f32)],
        name="finish",
        compiler_params=SMALL,
    )(band, fields)


def exchange_tiles(tiles, axis):
    return lax.all_to_all(tiles, axis, 0, 0, tiled=True)


def both_cores(chips):
    return lax.all_gather(chips, CORE, axis=0, tiled=False).reshape(-1, 128)


def per_device(orbitals):
    tile, copies = prepare(jnp.transpose(orbitals, (1, 0, 2)))
    own = exchange_tiles(copies, GRID)
    chips = lax.all_gather(lax.all_gather(tile, ("z4", "z2", "z1")), "xl").reshape(CHIPS, ROWS, 128)
    last = (jnp.asarray(LAST_HIGH), jnp.asarray(LAST_LOW))
    own, chips, *last = lax.optimization_barrier((own, chips, *last))
    pair, *made = lax.optimization_barrier((exchange_tiles(chips, GRID), *tables(*last)))
    pair = both_cores(pair)
    partial = partial_exchange(own.reshape(SLABS * ROWS, 128), pair, made)
    shares = exchange_tiles(partial.reshape(SLABS, ROWS, 128), GRID)
    field, lines = column_part(shares, both_cores(chips))
    parts = exchange_tiles(lines, GRID)
    fields = both_cores(exchange_tiles(attach(field, parts), PAIR))
    band = lax.axis_index(BAND).astype(jnp.int32).reshape(1)
    return jnp.transpose(finish(band, fields), (1, 0, 2))


def solution(mesh):
    parted = Mesh(mesh.devices.reshape((2,) * 9), BAND + GRID)
    spec = P(BAND, GRID, None)
    return jax.shard_map(per_device, mesh=parted, in_specs=(spec,), out_specs=spec, check_vma=False)
```

```python
import math

import jax
import jax.numpy as jnp
import numpy as np
from jax import lax
from jax.experimental import pallas as pl
from jax.experimental.pallas import tpu as pltpu
from jax.sharding import Mesh, PartitionSpec as P

NG = 48
BANDS = 32
COULOMB = 50.0
SLABS = 16
PLANES = NG // SLABS
COLS = NG * NG // 128
ROWS = 56
USED = PLANES * COLS
CHIPS = BANDS // 2
PAIR, CORE, GRID = ("xl", "z4", "z2", "z1"), ("c",), ("xh", "y4", "y2", "y1")
BAND = PAIR + CORE
PITCH = 56
f32, bf16 = jnp.float32, jnp.bfloat16
SMALL = pltpu.CompilerParams(vmem_limit_bytes=12 << 20)
LARGE = pltpu.CompilerParams(vmem_limit_bytes=24 << 20)


def real_basis():
    half = NG // 2
    freq = np.concatenate([np.arange(half + 1), np.arange(1, half)])
    turn = 2.0 * np.pi * ((freq[:, None] * np.arange(NG)[None, :]) % NG) / NG
    wave = np.where(np.arange(NG)[:, None] <= half, np.cos(turn), np.sin(turn))
    norm = np.where((np.arange(NG) == 0) | (np.arange(NG) == half), 1.0, 2.0) / NG
    return wave * np.sqrt(norm)[:, None], freq.astype(np.float64) ** 2


def halves(matrix):
    high = matrix.astype(np.float32).astype(bf16)
    low = (matrix - high.astype(np.float64)).astype(np.float32).astype(bf16)
    return high, low


def from_left(matrix):
    high, low = halves(matrix)
    return np.concatenate([high, high, low], 1)


BASIS, SQUARES = real_basis()
BASIS_X = BASIS[:, [PLANES * (r % SLABS) + r // SLABS for r in range(NG)]]
LEFTS = np.stack([from_left(m) for m in (BASIS_X, BASIS, BASIS.T, BASIS_X.T)])


def last_edge():
    wide = np.zeros((2, NG, 128))
    wide[0, :, :NG] = BASIS.T
    wide[1, :, 64 : 64 + NG] = BASIS.T
    return halves(wide)


LAST_HIGH, LAST_LOW = last_edge()


def split(x):
    high = x.astype(bf16)
    return high, (x - high.astype(f32)).astype(bf16)


def dot(a, b):
    return jnp.dot(a, b, preferred_element_type=f32)


def dot_t(a, b):
    return lax.dot_general(a, b, (((1,), (1,)), ((), ())), preferred_element_type=f32)


def left_mul(matrix, x):
    high, low = split(x)
    return dot(matrix, jnp.concatenate([high, low, high], 0))


def tables_kernel(high_ref, low_ref, wide_high, wide_low, coulomb):
    wide_high[...] = jnp.zeros_like(wide_high)
    wide_low[...] = jnp.zeros_like(wide_low)
    for w in range(2):
        for d in range(2):
            for i in range(4):
                rows = slice(48 * i + 64 * w, 48 * i + 64 * w + 48)
                cols = slice(128 * i, 128 * i + 128)
                wide_high[w, d, rows, cols] = high_ref[d]
                wide_low[w, d, rows, cols] = low_ref[d]

    def square(i):
        freq = jnp.where(i <= NG // 2, i, i - NG // 2).astype(f32)
        return freq * freq

    middle = lax.broadcasted_iota(jnp.int32, (NG, 128), 0)
    lane = lax.broadcasted_iota(jnp.int32, (NG, 128), 1)
    last = jnp.minimum(jnp.where(lane >= 64, lane - 64, lane), NG - 1)
    rest = square(middle) + square(last)
    for k in range(NG):
        total = rest + float(SQUARES[k])
        coulomb[k] = jnp.where(total > 0.0, -COULOMB / jnp.maximum(total, 1.0), 0.0)


def tables(last_high, last_low):
    wide = jax.ShapeDtypeStruct((2, 2, 256, 512), bf16)
    return pl.pallas_call(
        tables_kernel,
        out_shape=(wide, wide, jax.ShapeDtypeStruct((NG, NG, 128), f32)),
        name="tables",
        compiler_params=SMALL,
    )(last_high, last_low)


def exchange_kernel(
    own_ref, pair_ref, left_ref, wide_high, wide_low, coulomb, out_ref, rho_h, rho_l, za, zb, sol_h, sol_l
):
    def column(ref, first, c, step=ROWS):
        return jnp.concatenate(
            [ref[pl.ds(first + COLS * p + c, SLABS, stride=step), :] for p in range(PLANES)], 0
        )

    def partner(d, c):
        return column(pair_ref, d * SLABS * ROWS, c)

    def place(c):
        return slice(48 * (c // 3), 48 * (c // 3) + 48), slice(128 * (c % 3), 128 * (c % 3) + 128)

    for c in range(COLS):
        own = column(own_ref, 0, c, 2 * ROWS)
        rows, cols = place(c)
        for d in range(2):
            high, low = split(own * partner(d, c))
            rho_h[d, rows, cols] = high
            rho_l[d, rows, cols] = low
    for w in range(2):
        window = slice(128 * w, 128 * w + 256)
        out = None
        for d in range(2):
            high, low = rho_h[d, :, window], rho_l[d, :, window]
            term = dot(high, wide_high[w, d]) + dot(low, wide_high[w, d]) + dot(high, wide_low[w, d])
            out = term if out is None else out + term
        for c in range(6):
            for i in range(4):
                y = 8 * c + 4 * w + i
                za[PITCH * y : PITCH * y + NG, :] = out[48 * c : 48 * c + 48, 128 * i : 128 * i + 128]

    def planes(ref, k):
        return jnp.concatenate([ref[PITCH * i : PITCH * i + NG, :] for i in (k, k + 1)], 1)

    def across(ref, k):
        return jnp.concatenate([ref[pl.ds(i, NG, stride=PITCH), :] for i in (k, k + 1)], 1)

    def put(ref, k, both):
        for e in range(2):
            ref[PITCH * (k + e) : PITCH * (k + e) + NG, :] = both[:, 128 * e : 128 * e + 128]

    for y in range(0, NG, 2):
        put(zb, y, left_mul(left_ref[0], planes(za, y)))
    for k in range(0, NG, 2):
        both = left_mul(left_ref[1], across(zb, k)) * jnp.concatenate([coulomb[k], coulomb[k + 1]], 1)
        put(za, k, left_mul(left_ref[2], both))
    for y in range(0, NG, 2):
        both = left_mul(left_ref[3], across(za, y))
        for e in range(2):
            c, w, i = (y + e) // 8, ((y + e) % 8) // 4, (y + e) % 4
            high, low = split(both[:, 128 * e : 128 * e + 128])
            sol_h[w, 48 * c : 48 * c + 48, 128 * i : 128 * i + 128] = high
            sol_l[w, 48 * c : 48 * c + 48, 128 * i : 128 * i + 128] = low
    thirds = []
    for d in range(2):
        a, b = [
            dot_t(sol_h[w], wide_high[w, d]) + dot_t(sol_l[w], wide_high[w, d]) + dot_t(sol_h[w], wide_low[w, d])
            for w in range(2)
        ]
        thirds.append((a[:, :128], a[:, 128:] + b[:, :128], b[:, 128:]))
    for c in range(COLS):
        rows, _ = place(c)
        out = thirds[0][c % 3][rows] * partner(0, c)
        out = out + thirds[1][c % 3][rows] * partner(1, c)
        for p in range(PLANES):
            out_ref[pl.ds(COLS * p + c, SLABS, stride=ROWS), :] = out[16 * p : 16 * p + 16]
    for r in range(USED, ROWS):
        out_ref[pl.ds(r, SLABS, stride=ROWS), :] = jnp.zeros((SLABS, 128), f32)


def partial_exchange(own, pair, made):
    big = pltpu.VMEM((NG * PITCH, 128), f32)
    rho, solved = pltpu.VMEM((2, 288, 384), bf16), pltpu.VMEM((2, 288, 512), bf16)
    return pl.pallas_call(
        exchange_kernel,
        out_shape=jax.ShapeDtypeStruct((SLABS * ROWS, 128), f32),
        scratch_shapes=[rho, rho, big, big, solved, solved],
        name="exchange",
        compiler_params=LARGE,
    )(own, pair, jnp.asarray(LEFTS), *made)


def prepare_kernel(slab_ref, tile_ref, copies_ref):
    tile_ref[USED:ROWS, :] = jnp.zeros((ROWS - USED, 128), f32)
    for p in range(PLANES):
        for c in range(COLS):
            r = COLS * p + c
            tile_ref[r : r + 1, :] = slab_ref[p, :, 128 * c : 128 * c + 128]
    tile = tile_ref[...]
    for k in range(CHIPS):
        copies_ref[k] = tile


def prepare(slab):
    tile = jax.ShapeDtypeStruct((ROWS, 128), f32)
    copies = jax.ShapeDtypeStruct((CHIPS, ROWS, 128), f32)
    return pl.pallas_call(prepare_kernel, out_shape=(tile, copies), name="prepare", compiler_params=SMALL)(slab)


def join_kernel(tile_ref, chips_ref, out_ref):
    tile = tile_ref[...]
    for k in range(SLABS):
        out_ref[k, :ROWS, :] = tile
        out_ref[k, ROWS:, :] = chips_ref[k]


def join(tile, chips):
    return pl.pallas_call(
        join_kernel,
        out_shape=jax.ShapeDtypeStruct((SLABS, 2 * ROWS, 128), f32),
        name="join",
        compiler_params=SMALL,
    )(tile, chips)


def column_kernel(share_ref, orbital_ref, field_ref, copies_ref):
    field = jnp.sum(share_ref[...], axis=0)
    field_ref[...] = field
    sums = [
        jnp.sum(field * orbital_ref[ROWS * k : ROWS * k + ROWS, :], axis=0, keepdims=True) for k in range(BANDS)
    ]
    high, low = split(jnp.concatenate(sums + [jnp.zeros((128 - BANDS, 128), f32)], 0))
    ones = jnp.ones((8, 128), bf16)
    line = dot_t(ones, high) + dot_t(ones, low)
    for k in range(SLABS):
        copies_ref[k] = line


def column_part(shares, orbitals):
    field = jax.ShapeDtypeStruct((ROWS, 128), f32)
    copies = jax.ShapeDtypeStruct((SLABS, 8, 128), f32)
    return pl.pallas_call(column_kernel, out_shape=(field, copies), name="column", compiler_params=SMALL)(
        shares, orbitals
    )


def attach_kernel(field_ref, parts_ref, copies_ref):
    column = jnp.sum(parts_ref[...], axis=0)[:1]
    row = lax.broadcasted_iota(jnp.int32, (ROWS, 128), 0)
    tile = jnp.where(row == USED, column, field_ref[...])
    for k in range(CHIPS):
        copies_ref[k] = tile


def attach(field, parts):
    copies = jax.ShapeDtypeStruct((CHIPS, ROWS, 128), f32)
    return pl.pallas_call(attach_kernel, out_shape=copies, name="attach", compiler_params=SMALL)(field, parts)


BLOCK = 4


def place_of(band):
    return (band % 2) * CHIPS + band // 2


def finish_kernel(field_ref, out_ref, flat):
    mine = lax.axis_index(CORE + PAIR)
    matrix = field_ref[pl.ds(USED, BANDS, stride=ROWS), :][:, :BANDS]
    definite = (matrix + matrix.T) * (-0.5 / float(NG**3))
    row = lax.broadcasted_iota(jnp.int32, (BANDS, 2 * BANDS), 0)
    lane = lax.broadcasted_iota(jnp.int32, (BANDS, 2 * BANDS), 1)
    order = 2 * (row % CHIPS) + row // CHIPS
    unit = jnp.where(row[:, :BANDS] == lane[:, :BANDS], 1.0, 0.0).astype(f32)
    state = jnp.concatenate([definite, unit], 1)
    for first in range(0, BANDS, BLOCK):
        at = [place_of(first + i) for i in range(BLOCK)]
        columns = [jnp.broadcast_to(state[:, a : a + 1], (BANDS, 2 * BANDS)) for a in at]
        pivots = [state[a : a + 1, :] for a in at]
        for i in range(BLOCK):
            factor = jnp.where(order > first + i, columns[i] / columns[i][at[i] : at[i] + 1, :], 0.0)
            for j in range(i + 1, BLOCK):
                columns[j] = columns[j] - factor * columns[j][at[i] : at[i] + 1, :]
                pivots[j] = pivots[j] - factor[at[j] : at[j] + 1, :] * pivots[i]
            state = state - factor * pivots[i]
    picked = jnp.sum(jnp.where(row == mine, state, 0.0), axis=0, keepdims=True)
    pivot = jnp.sum(jnp.where(lane[:1] == mine, picked, 0.0), axis=1, keepdims=True)
    weights = picked * lax.rsqrt(pivot)
    total = None
    for k in range(BANDS):
        weight = weights[:, BANDS + k : BANDS + k + 1]
        term = weight * field_ref[ROWS * k : ROWS * k + ROWS, :]
        total = term if total is None else total + term
    flat[...] = total
    for p in range(PLANES):
        for c in range(COLS):
            r = COLS * p + c
            out_ref[p, :, 128 * c : 128 * c + 128] = flat[r : r + 1, :]


def finish(fields):
    return pl.pallas_call(
        finish_kernel,
        out_shape=jax.ShapeDtypeStruct((PLANES, 1, NG * NG), f32),
        scratch_shapes=[pltpu.VMEM((ROWS, 128), f32)],
        name="finish",
        compiler_params=SMALL,
    )(fields)


def exchange_tiles(tiles, axis):
    return lax.all_to_all(tiles, axis, 0, 0, tiled=True)


def both_cores(chips):
    return lax.all_gather(chips, CORE, axis=0, tiled=False).reshape(-1, 128)


def per_device(orbitals):
    tile, copies = prepare(jnp.transpose(orbitals, (1, 0, 2)))
    made = tables(jnp.asarray(LAST_HIGH), jnp.asarray(LAST_LOW))
    chips = exchange_tiles(copies, PAIR)
    whole = exchange_tiles(join(tile, chips), GRID)
    pair = both_cores(whole[:, ROWS:])
    partial = partial_exchange(whole.reshape(SLABS * 2 * ROWS, 128), pair, made)
    shares = exchange_tiles(partial.reshape(SLABS, ROWS, 128), GRID)
    field, lines = column_part(shares, both_cores(chips))
    parts = exchange_tiles(lines, GRID)
    fields = both_cores(exchange_tiles(attach(field, parts), PAIR))
    return jnp.transpose(finish(fields), (1, 0, 2))


def solution(mesh):
    parted = Mesh(mesh.devices.reshape((2,) * 9), BAND + GRID)
    spec = P(BAND, GRID, None)
    return jax.shard_map(per_device, mesh=parted, in_specs=(spec,), out_specs=spec, check_vma=False)
```

```python
import math

import jax
import jax.numpy as jnp
import numpy as np
from jax import lax
from jax.experimental import pallas as pl
from jax.experimental.pallas import tpu as pltpu
from jax.sharding import Mesh, PartitionSpec as P

NG = 48
BANDS = 32
COULOMB = 50.0
SLABS = 16
PLANES = NG // SLABS
COLS = NG * NG // 128
ROWS = 56
USED = PLANES * COLS
CHIPS = BANDS // 2
PAIR, CORE, GRID = ("xl", "z4", "z2", "z1"), ("c",), ("xh", "y4", "y2", "y1")
BAND = PAIR + CORE
PITCH = 56
f32, bf16 = jnp.float32, jnp.bfloat16
SMALL = pltpu.CompilerParams(vmem_limit_bytes=12 << 20)
LARGE = pltpu.CompilerParams(vmem_limit_bytes=24 << 20)


def real_basis():
    half = NG // 2
    freq = np.concatenate([np.arange(half + 1), np.arange(1, half)])
    turn = 2.0 * np.pi * ((freq[:, None] * np.arange(NG)[None, :]) % NG) / NG
    wave = np.where(np.arange(NG)[:, None] <= half, np.cos(turn), np.sin(turn))
    norm = np.where((np.arange(NG) == 0) | (np.arange(NG) == half), 1.0, 2.0) / NG
    return wave * np.sqrt(norm)[:, None], freq.astype(np.float64) ** 2


def halves(matrix):
    high = matrix.astype(np.float32).astype(bf16)
    low = (matrix - high.astype(np.float64)).astype(np.float32).astype(bf16)
    return high, low


def from_left(matrix):
    high, low = halves(matrix)
    return np.concatenate([high, high, low], 1)


BASIS, SQUARES = real_basis()
BASIS_X = BASIS[:, [PLANES * (r % SLABS) + r // SLABS for r in range(NG)]]
LEFTS = np.stack([from_left(m) for m in (BASIS_X, BASIS, BASIS.T, BASIS_X.T)])


def last_edge():
    wide = np.zeros((2, NG, 128))
    wide[0, :, :NG] = BASIS.T
    wide[1, :, 64 : 64 + NG] = BASIS.T
    return halves(wide)


LAST_HIGH, LAST_LOW = last_edge()


def split(x):
    high = x.astype(bf16)
    return high, (x - high.astype(f32)).astype(bf16)


def dot(a, b):
    return jnp.dot(a, b, preferred_element_type=f32)


def dot_t(a, b):
    return lax.dot_general(a, b, (((1,), (1,)), ((), ())), preferred_element_type=f32)


def left_mul(matrix, x):
    high, low = split(x)
    return dot(matrix, jnp.concatenate([high, low, high], 0))


def tables_kernel(high_ref, low_ref, wide_high, wide_low, coulomb):
    wide_high[...] = jnp.zeros_like(wide_high)
    wide_low[...] = jnp.zeros_like(wide_low)
    for w in range(2):
        for d in range(2):
            for i in range(4):
                rows = slice(48 * i + 64 * w, 48 * i + 64 * w + 48)
                cols = slice(128 * i, 128 * i + 128)
                wide_high[w, d, rows, cols] = high_ref[d]
                wide_low[w, d, rows, cols] = low_ref[d]

    def square(i):
        freq = jnp.where(i <= NG // 2, i, i - NG // 2).astype(f32)
        return freq * freq

    middle = lax.broadcasted_iota(jnp.int32, (NG, 128), 0)
    lane = lax.broadcasted_iota(jnp.int32, (NG, 128), 1)
    last = jnp.minimum(jnp.where(lane >= 64, lane - 64, lane), NG - 1)
    rest = square(middle) + square(last)
    for k in range(NG):
        total = rest + float(SQUARES[k])
        coulomb[k] = jnp.where(total > 0.0, -COULOMB / jnp.maximum(total, 1.0), 0.0)


def tables(last_high, last_low):
    wide = jax.ShapeDtypeStruct((2, 2, 256, 512), bf16)
    return pl.pallas_call(
        tables_kernel,
        out_shape=(wide, wide, jax.ShapeDtypeStruct((NG, NG, 128), f32)),
        name="tables",
        compiler_params=SMALL,
    )(last_high, last_low)


def exchange_kernel(
    own_ref, pair_ref, left_ref, wide_high, wide_low, coulomb, out_ref, rho_h, rho_l, za, zb, sol_h, sol_l
):
    def column(ref, first, c, step=ROWS):
        return jnp.concatenate(
            [ref[pl.ds(first + COLS * p + c, SLABS, stride=step), :] for p in range(PLANES)], 0
        )

    def partner(d, c):
        return column(pair_ref, d * SLABS * ROWS, c)

    def rows_of(c):
        return pl.ds(pl.multiple_of(NG * c, 16), NG)

    def densities(c, _):
        for k in range(3):
            own = column(own_ref, 0, 3 * c + k, 2 * ROWS)
            for d in range(2):
                high, low = split(own * partner(d, 3 * c + k))
                rho_h[d, rows_of(c), 128 * k : 128 * k + 128] = high
                rho_l[d, rows_of(c), 128 * k : 128 * k + 128] = low
        return 0

    lax.fori_loop(0, 6, densities, 0)
    for w in range(2):
        window = slice(128 * w, 128 * w + 256)
        out = None
        for d in range(2):
            high, low = rho_h[d, :, window], rho_l[d, :, window]
            term = dot(high, wide_high[w, d]) + dot(low, wide_high[w, d]) + dot(high, wide_low[w, d])
            out = term if out is None else out + term
        for c in range(6):
            for i in range(4):
                y = 8 * c + 4 * w + i
                za[PITCH * y : PITCH * y + NG, :] = out[48 * c : 48 * c + 48, 128 * i : 128 * i + 128]

    def plane(k):
        return pl.ds(pl.multiple_of(PITCH * k, 8), NG)

    def planes(ref, k):
        return jnp.concatenate([ref[plane(k), :], ref[plane(k + 1), :]], 1)

    def across(ref, k):
        return jnp.concatenate([ref[pl.ds(i, NG, stride=PITCH), :] for i in (k, k + 1)], 1)

    def put(ref, k, both):
        for e in range(2):
            ref[plane(k + e), :] = both[:, 128 * e : 128 * e + 128]

    def first_edge(c, _):
        for j in range(0, 8, 2):
            put(zb, 8 * c + j, left_mul(left_ref[0], planes(za, 8 * c + j)))
        return 0

    def middle_edge(c, _):
        for j in range(0, 8, 2):
            k = 8 * c + j
            both = left_mul(left_ref[1], across(zb, k)) * jnp.concatenate([coulomb[k], coulomb[k + 1]], 1)
            put(za, k, left_mul(left_ref[2], both))
        return 0

    def first_edge_back(c, _):
        for j in range(0, 8, 2):
            both = left_mul(left_ref[3], across(za, 8 * c + j))
            for e in range(2):
                w, i = (j + e) // 4, (j + e) % 4
                high, low = split(both[:, 128 * e : 128 * e + 128])
                sol_h[w, rows_of(c), 128 * i : 128 * i + 128] = high
                sol_l[w, rows_of(c), 128 * i : 128 * i + 128] = low
        return 0

    lax.fori_loop(0, 6, first_edge, 0)
    lax.fori_loop(0, 6, middle_edge, 0)
    lax.fori_loop(0, 6, first_edge_back, 0)
    thirds = []
    for d in range(2):
        a, b = [
            dot_t(sol_h[w], wide_high[w, d]) + dot_t(sol_l[w], wide_high[w, d]) + dot_t(sol_h[w], wide_low[w, d])
            for w in range(2)
        ]
        thirds.append((a[:, :128], a[:, 128:] + b[:, :128], b[:, 128:]))
    for c in range(COLS):
        rows = slice(48 * (c // 3), 48 * (c // 3) + 48)
        out = thirds[0][c % 3][rows] * partner(0, c)
        out = out + thirds[1][c % 3][rows] * partner(1, c)
        for p in range(PLANES):
            out_ref[pl.ds(COLS * p + c, SLABS, stride=ROWS), :] = out[16 * p : 16 * p + 16]
    for r in range(USED, ROWS):
        out_ref[pl.ds(r, SLABS, stride=ROWS), :] = jnp.zeros((SLABS, 128), f32)


def partial_exchange(own, pair, made):
    big = pltpu.VMEM((NG * PITCH, 128), f32)
    rho, solved = pltpu.VMEM((2, 288, 384), bf16), pltpu.VMEM((2, 288, 512), bf16)
    return pl.pallas_call(
        exchange_kernel,
        out_shape=jax.ShapeDtypeStruct((SLABS * ROWS, 128), f32),
        scratch_shapes=[rho, rho, big, big, solved, solved],
        name="exchange",
        compiler_params=LARGE,
    )(own, pair, jnp.asarray(LEFTS), *made)


def prepare_kernel(slab_ref, tile_ref, copies_ref):
    tile_ref[USED:ROWS, :] = jnp.zeros((ROWS - USED, 128), f32)
    for p in range(PLANES):
        for c in range(COLS):
            r = COLS * p + c
            tile_ref[r : r + 1, :] = slab_ref[p, :, 128 * c : 128 * c + 128]
    tile = tile_ref[...]
    for k in range(CHIPS):
        copies_ref[k] = tile


def prepare(slab):
    tile = jax.ShapeDtypeStruct((ROWS, 128), f32)
    copies = jax.ShapeDtypeStruct((CHIPS, ROWS, 128), f32)
    return pl.pallas_call(prepare_kernel, out_shape=(tile, copies), name="prepare", compiler_params=SMALL)(slab)


def join_kernel(tile_ref, chips_ref, out_ref):
    tile = tile_ref[...]
    for k in range(SLABS):
        out_ref[k, :ROWS, :] = tile
        out_ref[k, ROWS:, :] = chips_ref[k]


def join(tile, chips):
    return pl.pallas_call(
        join_kernel,
        out_shape=jax.ShapeDtypeStruct((SLABS, 2 * ROWS, 128), f32),
        name="join",
        compiler_params=SMALL,
    )(tile, chips)


def column_kernel(share_ref, orbital_ref, field_ref, copies_ref):
    field = jnp.sum(share_ref[...], axis=0)
    field_ref[...] = field
    sums = [
        jnp.sum(field * orbital_ref[ROWS * k : ROWS * k + ROWS, :], axis=0, keepdims=True) for k in range(BANDS)
    ]
    high, low = split(jnp.concatenate(sums + [jnp.zeros((128 - BANDS, 128), f32)], 0))
    ones = jnp.ones((8, 128), bf16)
    line = dot_t(ones, high) + dot_t(ones, low)
    for k in range(SLABS):
        copies_ref[k] = line


def column_part(shares, orbitals):
    field = jax.ShapeDtypeStruct((ROWS, 128), f32)
    copies = jax.ShapeDtypeStruct((SLABS, 8, 128), f32)
    return pl.pallas_call(column_kernel, out_shape=(field, copies), name="column", compiler_params=SMALL)(
        shares, orbitals
    )


def attach_kernel(field_ref, parts_ref, copies_ref):
    column = jnp.sum(parts_ref[...], axis=0)[:1]
    row = lax.broadcasted_iota(jnp.int32, (ROWS, 128), 0)
    tile = jnp.where(row == USED, column, field_ref[...])
    for k in range(CHIPS):
        copies_ref[k] = tile


def attach(field, parts):
    copies = jax.ShapeDtypeStruct((CHIPS, ROWS, 128), f32)
    return pl.pallas_call(attach_kernel, out_shape=copies, name="attach", compiler_params=SMALL)(field, parts)


BLOCK = 4


def place_of(band):
    return (band % 2) * CHIPS + band // 2


def finish_kernel(field_ref, out_ref, flat):
    mine = lax.axis_index(CORE + PAIR)
    matrix = field_ref[pl.ds(USED, BANDS, stride=ROWS), :][:, :BANDS]
    definite = (matrix + matrix.T) * (-0.5 / float(NG**3))
    row = lax.broadcasted_iota(jnp.int32, (BANDS, 2 * BANDS), 0)
    lane = lax.broadcasted_iota(jnp.int32, (BANDS, 2 * BANDS), 1)
    order = 2 * (row % CHIPS) + row // CHIPS
    unit = jnp.where(row[:, :BANDS] == lane[:, :BANDS], 1.0, 0.0).astype(f32)
    state = jnp.concatenate([definite, unit], 1)
    for first in range(0, BANDS, BLOCK):
        at = [place_of(first + i) for i in range(BLOCK)]
        columns = [jnp.broadcast_to(state[:, a : a + 1], (BANDS, 2 * BANDS)) for a in at]
        pivots = [state[a : a + 1, :] for a in at]
        for i in range(BLOCK):
            factor = jnp.where(order > first + i, columns[i] / columns[i][at[i] : at[i] + 1, :], 0.0)
            for j in range(i + 1, BLOCK):
                columns[j] = columns[j] - factor * columns[j][at[i] : at[i] + 1, :]
                pivots[j] = pivots[j] - factor[at[j] : at[j] + 1, :] * pivots[i]
            state = state - factor * pivots[i]
    picked = jnp.sum(jnp.where(row == mine, state, 0.0), axis=0, keepdims=True)
    pivot = jnp.sum(jnp.where(lane[:1] == mine, picked, 0.0), axis=1, keepdims=True)
    weights = picked * lax.rsqrt(pivot)
    total = None
    for k in range(BANDS):
        weight = weights[:, BANDS + k : BANDS + k + 1]
        term = weight * field_ref[ROWS * k : ROWS * k + ROWS, :]
        total = term if total is None else total + term
    flat[...] = total
    for p in range(PLANES):
        for c in range(COLS):
            r = COLS * p + c
            out_ref[p, :, 128 * c : 128 * c + 128] = flat[r : r + 1, :]


def finish(fields):
    return pl.pallas_call(
        finish_kernel,
        out_shape=jax.ShapeDtypeStruct((PLANES, 1, NG * NG), f32),
        scratch_shapes=[pltpu.VMEM((ROWS, 128), f32)],
        name="finish",
        compiler_params=SMALL,
    )(fields)


def exchange_tiles(tiles, axis):
    return lax.all_to_all(tiles, axis, 0, 0, tiled=True)


def both_cores(chips):
    return lax.all_gather(chips, CORE, axis=0, tiled=False).reshape(-1, 128)


def per_device(orbitals):
    tile, copies = prepare(jnp.transpose(orbitals, (1, 0, 2)))
    made = tables(jnp.asarray(LAST_HIGH), jnp.asarray(LAST_LOW))
    chips = exchange_tiles(copies, PAIR)
    whole, others = lax.optimization_barrier((exchange_tiles(join(tile, chips), GRID), both_cores(chips)))
    pair = both_cores(whole[:, ROWS:])
    partial = partial_exchange(whole.reshape(SLABS * 2 * ROWS, 128), pair, made)
    shares = exchange_tiles(partial.reshape(SLABS, ROWS, 128), GRID)
    field, lines = column_part(shares, others)
    parts = exchange_tiles(lines, GRID)
    fields = both_cores(exchange_tiles(attach(field, parts), PAIR))
    return jnp.transpose(finish(fields), (1, 0, 2))


def solution(mesh):
    parted = Mesh(mesh.devices.reshape((2,) * 9), BAND + GRID)
    spec = P(BAND, GRID, None)
    return jax.shard_map(per_device, mesh=parted, in_specs=(spec,), out_specs=spec, check_vma=False)
```

```python
import math

import jax
import jax.numpy as jnp
import numpy as np
from jax import lax
from jax.experimental import pallas as pl
from jax.experimental.pallas import tpu as pltpu
from jax.sharding import Mesh, PartitionSpec as P

NG = 48
BANDS = 32
COULOMB = 50.0
SLABS = 16
PLANES = NG // SLABS
COLS = NG * NG // 128
ROWS = 56
USED = PLANES * COLS
CHIPS = BANDS // 2
PAIR, CORE, GRID = ("xl", "z4", "z2", "z1"), ("c",), ("xh", "y4", "y2", "y1")
BAND = PAIR + CORE
PITCH = 56
f32, bf16 = jnp.float32, jnp.bfloat16
SMALL = pltpu.CompilerParams(vmem_limit_bytes=12 << 20)
LARGE = pltpu.CompilerParams(vmem_limit_bytes=24 << 20)


def real_basis():
    half = NG // 2
    freq = np.concatenate([np.arange(half + 1), np.arange(1, half)])
    turn = 2.0 * np.pi * ((freq[:, None] * np.arange(NG)[None, :]) % NG) / NG
    wave = np.where(np.arange(NG)[:, None] <= half, np.cos(turn), np.sin(turn))
    norm = np.where((np.arange(NG) == 0) | (np.arange(NG) == half), 1.0, 2.0) / NG
    return wave * np.sqrt(norm)[:, None], freq.astype(np.float64) ** 2


def halves(matrix):
    high = matrix.astype(np.float32).astype(bf16)
    low = (matrix - high.astype(np.float64)).astype(np.float32).astype(bf16)
    return high, low


def from_left(matrix):
    high, low = halves(matrix)
    return np.concatenate([high, high, low], 1)


BASIS, SQUARES = real_basis()
BASIS_X = BASIS[:, [PLANES * (r % SLABS) + r // SLABS for r in range(NG)]]
LEFTS = np.stack([from_left(m) for m in (BASIS_X, BASIS, BASIS.T, BASIS_X.T)])


def last_edge():
    wide = np.zeros((2, NG, 128))
    wide[0, :, :NG] = BASIS.T
    wide[1, :, 64 : 64 + NG] = BASIS.T
    return halves(wide)


LAST_HIGH, LAST_LOW = last_edge()


def split(x):
    high = x.astype(bf16)
    return high, (x - high.astype(f32)).astype(bf16)


def dot(a, b):
    return jnp.dot(a, b, preferred_element_type=f32)


def dot_t(a, b):
    return lax.dot_general(a, b, (((1,), (1,)), ((), ())), preferred_element_type=f32)


def left_mul(matrix, x):
    high, low = split(x)
    return dot(matrix, jnp.concatenate([high, low, high], 0))


def tables_kernel(high_ref, low_ref, wide_high, wide_low, coulomb):
    wide_high[...] = jnp.zeros_like(wide_high)
    wide_low[...] = jnp.zeros_like(wide_low)
    for w in range(2):
        for d in range(2):
            for i in range(4):
                rows = slice(48 * i + 64 * w, 48 * i + 64 * w + 48)
                cols = slice(128 * i, 128 * i + 128)
                wide_high[w, d, rows, cols] = high_ref[d]
                wide_low[w, d, rows, cols] = low_ref[d]

    def square(i):
        freq = jnp.where(i <= NG // 2, i, i - NG // 2).astype(f32)
        return freq * freq

    middle = lax.broadcasted_iota(jnp.int32, (NG, 128), 0)
    lane = lax.broadcasted_iota(jnp.int32, (NG, 128), 1)
    last = jnp.minimum(jnp.where(lane >= 64, lane - 64, lane), NG - 1)
    rest = square(middle) + square(last)
    for k in range(NG):
        total = rest + float(SQUARES[k])
        coulomb[k] = jnp.where(total > 0.0, -COULOMB / jnp.maximum(total, 1.0), 0.0)


def tables(last_high, last_low):
    wide = jax.ShapeDtypeStruct((2, 2, 256, 512), bf16)
    return pl.pallas_call(
        tables_kernel,
        out_shape=(wide, wide, jax.ShapeDtypeStruct((NG, NG, 128), f32)),
        name="tables",
        compiler_params=SMALL,
    )(last_high, last_low)


HALF = 6 * NG


def folded(x):
    return x[:HALF] + x[HALF:]


def exchange_kernel(
    own_ref, pair_ref, left_ref, wide_high, wide_low, coulomb, out_ref, rho, za, zb, solved
):
    def column(ref, first, c, step=ROWS):
        return jnp.concatenate(
            [ref[pl.ds(first + COLS * p + c, SLABS, stride=step), :] for p in range(PLANES)], 0
        )

    def partner(d, c):
        return column(pair_ref, d * SLABS * ROWS, c)

    def place(c):
        return slice(48 * (c // 3), 48 * (c // 3) + 48), slice(128 * (c % 3), 128 * (c % 3) + 128)

    for c in range(COLS):
        own = column(own_ref, 0, c, 2 * ROWS)
        rows, cols = place(c)
        for d in range(2):
            high, low = split(own * partner(d, c))
            rho[d, rows, cols] = high
            rho[d, slice(HALF + rows.start, HALF + rows.stop), cols] = low
    for w in range(2):
        window = slice(128 * w, 128 * w + 256)
        out = None
        for d in range(2):
            both = dot(rho[d, :, window], wide_high[w, d])
            term = folded(both) + dot(rho[d, :HALF, window], wide_low[w, d])
            out = term if out is None else out + term
        for c in range(6):
            for i in range(4):
                y = 8 * c + 4 * w + i
                za[PITCH * y : PITCH * y + NG, :] = out[48 * c : 48 * c + 48, 128 * i : 128 * i + 128]

    def planes(ref, k):
        return jnp.concatenate([ref[PITCH * i : PITCH * i + NG, :] for i in (k, k + 1)], 1)

    def across(ref, k):
        return jnp.concatenate([ref[pl.ds(i, NG, stride=PITCH), :] for i in (k, k + 1)], 1)

    def put(ref, k, both):
        for e in range(2):
            ref[PITCH * (k + e) : PITCH * (k + e) + NG, :] = both[:, 128 * e : 128 * e + 128]

    for y in range(0, NG, 2):
        put(zb, y, left_mul(left_ref[0], planes(za, y)))
    for k in range(0, NG, 2):
        both = left_mul(left_ref[1], across(zb, k)) * jnp.concatenate([coulomb[k], coulomb[k + 1]], 1)
        put(za, k, left_mul(left_ref[2], both))
    for y in range(0, NG, 2):
        both = left_mul(left_ref[3], across(za, y))
        for e in range(2):
            c, w, i = (y + e) // 8, ((y + e) % 8) // 4, (y + e) % 4
            high, low = split(both[:, 128 * e : 128 * e + 128])
            solved[w, 48 * c : 48 * c + 48, 128 * i : 128 * i + 128] = high
            solved[w, HALF + 48 * c : HALF + 48 * c + 48, 128 * i : 128 * i + 128] = low
    thirds = []
    for d in range(2):
        a, b = [
            folded(dot_t(solved[w], wide_high[w, d])) + dot_t(solved[w, :HALF], wide_low[w, d]) for w in range(2)
        ]
        thirds.append((a[:, :128], a[:, 128:] + b[:, :128], b[:, 128:]))
    for c in range(COLS):
        rows, _ = place(c)
        out = thirds[0][c % 3][rows] * partner(0, c)
        out = out + thirds[1][c % 3][rows] * partner(1, c)
        for p in range(PLANES):
            out_ref[pl.ds(COLS * p + c, SLABS, stride=ROWS), :] = out[16 * p : 16 * p + 16]
    for r in range(USED, ROWS):
        out_ref[pl.ds(r, SLABS, stride=ROWS), :] = jnp.zeros((SLABS, 128), f32)


def partial_exchange(own, pair, made):
    big = pltpu.VMEM((NG * PITCH, 128), f32)
    rho, solved = pltpu.VMEM((2, 2 * HALF, 384), bf16), pltpu.VMEM((2, 2 * HALF, 512), bf16)
    return pl.pallas_call(
        exchange_kernel,
        out_shape=jax.ShapeDtypeStruct((SLABS * ROWS, 128), f32),
        scratch_shapes=[rho, big, big, solved],
        name="exchange",
        compiler_params=LARGE,
    )(own, pair, jnp.asarray(LEFTS), *made)


def prepare_kernel(slab_ref, tile_ref, copies_ref):
    tile_ref[USED:ROWS, :] = jnp.zeros((ROWS - USED, 128), f32)
    for p in range(PLANES):
        for c in range(COLS):
            r = COLS * p + c
            tile_ref[r : r + 1, :] = slab_ref[p, :, 128 * c : 128 * c + 128]
    tile = tile_ref[...]
    for k in range(CHIPS):
        copies_ref[k] = tile


def prepare(slab):
    tile = jax.ShapeDtypeStruct((ROWS, 128), f32)
    copies = jax.ShapeDtypeStruct((CHIPS, ROWS, 128), f32)
    return pl.pallas_call(prepare_kernel, out_shape=(tile, copies), name="prepare", compiler_params=SMALL)(slab)


def join_kernel(tile_ref, chips_ref, out_ref):
    tile = tile_ref[...]
    for k in range(SLABS):
        out_ref[k, :ROWS, :] = tile
        out_ref[k, ROWS:, :] = chips_ref[k]


def join(tile, chips):
    return pl.pallas_call(
        join_kernel,
        out_shape=jax.ShapeDtypeStruct((SLABS, 2 * ROWS, 128), f32),
        name="join",
        compiler_params=SMALL,
    )(tile, chips)


def column_kernel(share_ref, orbital_ref, field_ref, copies_ref):
    field = jnp.sum(share_ref[...], axis=0)
    field_ref[...] = field
    sums = [
        jnp.sum(field * orbital_ref[ROWS * k : ROWS * k + ROWS, :], axis=0, keepdims=True) for k in range(BANDS)
    ]
    high, low = split(jnp.concatenate(sums + [jnp.zeros((128 - BANDS, 128), f32)], 0))
    ones = jnp.ones((8, 128), bf16)
    line = dot_t(ones, high) + dot_t(ones, low)
    for k in range(SLABS):
        copies_ref[k] = line


def column_part(shares, orbitals):
    field = jax.ShapeDtypeStruct((ROWS, 128), f32)
    copies = jax.ShapeDtypeStruct((SLABS, 8, 128), f32)
    return pl.pallas_call(column_kernel, out_shape=(field, copies), name="column", compiler_params=SMALL)(
        shares, orbitals
    )


def attach_kernel(field_ref, parts_ref, copies_ref):
    column = jnp.sum(parts_ref[...], axis=0)[:1]
    row = lax.broadcasted_iota(jnp.int32, (ROWS, 128), 0)
    tile = jnp.where(row == USED, column, field_ref[...])
    for k in range(CHIPS):
        copies_ref[k] = tile


def attach(field, parts):
    copies = jax.ShapeDtypeStruct((CHIPS, ROWS, 128), f32)
    return pl.pallas_call(attach_kernel, out_shape=copies, name="attach", compiler_params=SMALL)(field, parts)


BLOCK = 8


def place_of(band):
    return (band % 2) * CHIPS + band // 2


def finish_kernel(field_ref, out_ref, flat):
    mine = lax.axis_index(CORE + PAIR)
    matrix = field_ref[pl.ds(USED, BANDS, stride=ROWS), :][:, :BANDS]
    definite = (matrix + matrix.T) * (-0.5 / float(NG**3))
    row = lax.broadcasted_iota(jnp.int32, (BANDS, 2 * BANDS), 0)
    lane = lax.broadcasted_iota(jnp.int32, (BANDS, 2 * BANDS), 1)
    order = 2 * (row % CHIPS) + row // CHIPS
    unit = jnp.where(row[:, :BANDS] == lane[:, :BANDS], 1.0, 0.0).astype(f32)
    state = jnp.concatenate([definite, unit], 1)
    for first in range(0, BANDS, BLOCK):
        at = [place_of(first + i) for i in range(BLOCK)]
        columns = [jnp.broadcast_to(state[:, a : a + 1], (BANDS, 2 * BANDS)) for a in at]
        pivots = [state[a : a + 1, :] for a in at]
        for i in range(BLOCK):
            factor = jnp.where(order > first + i, columns[i] / columns[i][at[i] : at[i] + 1, :], 0.0)
            for j in range(i + 1, BLOCK):
                columns[j] = columns[j] - factor * columns[j][at[i] : at[i] + 1, :]
                pivots[j] = pivots[j] - factor[at[j] : at[j] + 1, :] * pivots[i]
            state = state - factor * pivots[i]
    picked = jnp.sum(jnp.where(row == mine, state, 0.0), axis=0, keepdims=True)
    pivot = jnp.sum(jnp.where(lane[:1] == mine, picked, 0.0), axis=1, keepdims=True)
    weights = picked * lax.rsqrt(pivot)
    total = None
    for k in range(BANDS):
        weight = weights[:, BANDS + k : BANDS + k + 1]
        term = weight * field_ref[ROWS * k : ROWS * k + ROWS, :]
        total = term if total is None else total + term
    flat[...] = total
    for p in range(PLANES):
        for c in range(COLS):
            r = COLS * p + c
            out_ref[p, :, 128 * c : 128 * c + 128] = flat[r : r + 1, :]


def finish(fields):
    return pl.pallas_call(
        finish_kernel,
        out_shape=jax.ShapeDtypeStruct((PLANES, 1, NG * NG), f32),
        scratch_shapes=[pltpu.VMEM((ROWS, 128), f32)],
        name="finish",
        compiler_params=SMALL,
    )(fields)


def exchange_tiles(tiles, axis):
    return lax.all_to_all(tiles, axis, 0, 0, tiled=True)


def both_cores(chips):
    return lax.all_gather(chips, CORE, axis=0, tiled=False).reshape(-1, 128)


def per_device(orbitals):
    tile, copies = prepare(jnp.transpose(orbitals, (1, 0, 2)))
    made = tables(jnp.asarray(LAST_HIGH), jnp.asarray(LAST_LOW))
    chips = exchange_tiles(copies, PAIR)
    whole, others = lax.optimization_barrier((exchange_tiles(join(tile, chips), GRID), both_cores(chips)))
    pair = both_cores(whole[:, ROWS:])
    partial = partial_exchange(whole.reshape(SLABS * 2 * ROWS, 128), pair, made)
    shares = exchange_tiles(partial.reshape(SLABS, ROWS, 128), GRID)
    field, lines = column_part(shares, others)
    parts = exchange_tiles(lines, GRID)
    fields = both_cores(exchange_tiles(attach(field, parts), PAIR))
    return jnp.transpose(finish(fields), (1, 0, 2))


def solution(mesh):
    parted = Mesh(mesh.devices.reshape((2,) * 9), BAND + GRID)
    spec = P(BAND, GRID, None)
    return jax.shard_map(per_device, mesh=parted, in_specs=(spec,), out_specs=spec, check_vma=False)
```

```python
import math

import jax
import jax.numpy as jnp
import numpy as np
from jax import lax
from jax.experimental import pallas as pl
from jax.experimental.pallas import tpu as pltpu
from jax.sharding import Mesh, PartitionSpec as P

NG = 48
BANDS = 32
COULOMB = 50.0
SLABS = 16
PLANES = NG // SLABS
COLS = NG * NG // 128
ROWS = 56
USED = PLANES * COLS
CHIPS = BANDS // 2
PAIR, CORE, GRID = ("xl", "z4", "z2", "z1"), ("c",), ("xh", "y4", "y2", "y1")
BAND = PAIR + CORE
CROSS = ("xl",) + GRID
ROLES = [[(q ^ h) * 16 + h * 8 + y for h in range(2) for y in range(8)] for q in range(2)]
PITCH = 56
f32, bf16 = jnp.float32, jnp.bfloat16
SMALL = pltpu.CompilerParams(vmem_limit_bytes=12 << 20)
LARGE = pltpu.CompilerParams(vmem_limit_bytes=24 << 20)


def real_basis():
    half = NG // 2
    freq = np.concatenate([np.arange(half + 1), np.arange(1, half)])
    turn = 2.0 * np.pi * ((freq[:, None] * np.arange(NG)[None, :]) % NG) / NG
    wave = np.where(np.arange(NG)[:, None] <= half, np.cos(turn), np.sin(turn))
    norm = np.where((np.arange(NG) == 0) | (np.arange(NG) == half), 1.0, 2.0) / NG
    return wave * np.sqrt(norm)[:, None], freq.astype(np.float64) ** 2


def halves(matrix):
    high = matrix.astype(np.float32).astype(bf16)
    low = (matrix - high.astype(np.float64)).astype(np.float32).astype(bf16)
    return high, low


def from_left(matrix):
    high, low = halves(matrix)
    return np.concatenate([high, high, low], 1)


BASIS, SQUARES = real_basis()
BASIS_X = BASIS[:, [PLANES * (r % SLABS) + r // SLABS for r in range(NG)]]
LEFTS = np.stack([from_left(m) for m in (BASIS_X, BASIS, BASIS.T, BASIS_X.T)])


def last_edge():
    wide = np.zeros((2, NG, 128))
    wide[0, :, :NG] = BASIS.T
    wide[1, :, 64 : 64 + NG] = BASIS.T
    return halves(wide)


LAST_HIGH, LAST_LOW = last_edge()


def split(x):
    high = x.astype(bf16)
    return high, (x - high.astype(f32)).astype(bf16)


def dot(a, b):
    return jnp.dot(a, b, preferred_element_type=f32)


def dot_t(a, b):
    return lax.dot_general(a, b, (((1,), (1,)), ((), ())), preferred_element_type=f32)


def left_mul(matrix, x):
    high, low = split(x)
    return dot(matrix, jnp.concatenate([high, low, high], 0))


def tables_kernel(high_ref, low_ref, wide_high, wide_low, coulomb):
    wide_high[...] = jnp.zeros_like(wide_high)
    wide_low[...] = jnp.zeros_like(wide_low)
    for w in range(2):
        for d in range(2):
            for i in range(4):
                rows = slice(48 * i + 64 * w, 48 * i + 64 * w + 48)
                cols = slice(128 * i, 128 * i + 128)
                wide_high[w, d, rows, cols] = high_ref[d]
                wide_low[w, d, rows, cols] = low_ref[d]

    def square(i):
        freq = jnp.where(i <= NG // 2, i, i - NG // 2).astype(f32)
        return freq * freq

    middle = lax.broadcasted_iota(jnp.int32, (NG, 128), 0)
    lane = lax.broadcasted_iota(jnp.int32, (NG, 128), 1)
    last = jnp.minimum(jnp.where(lane >= 64, lane - 64, lane), NG - 1)
    rest = square(middle) + square(last)
    for k in range(NG):
        total = rest + float(SQUARES[k])
        coulomb[k] = jnp.where(total > 0.0, -COULOMB / jnp.maximum(total, 1.0), 0.0)


def tables(last_high, last_low):
    wide = jax.ShapeDtypeStruct((2, 2, 256, 512), bf16)
    return pl.pallas_call(
        tables_kernel,
        out_shape=(wide, wide, jax.ShapeDtypeStruct((NG, NG, 128), f32)),
        name="tables",
        compiler_params=SMALL,
    )(last_high, last_low)


HALF = 6 * NG


def folded(x):
    return x[:HALF] + x[HALF:]


def exchange_kernel(
    own_ref, pair_ref, left_ref, wide_high, wide_low, coulomb, out_ref, rho, za, zb, solved
):
    def column(ref, first, c, step=ROWS):
        return jnp.concatenate(
            [ref[pl.ds(first + COLS * p + c, SLABS, stride=step), :] for p in range(PLANES)], 0
        )

    def partner(d, c):
        return column(pair_ref, d * SLABS * ROWS, c)

    def place(c):
        return slice(48 * (c // 3), 48 * (c // 3) + 48), slice(128 * (c % 3), 128 * (c % 3) + 128)

    for c in range(COLS):
        own = column(own_ref, 0, c, 2 * ROWS)
        rows, cols = place(c)
        for d in range(2):
            high, low = split(own * partner(d, c))
            rho[d, rows, cols] = high
            rho[d, slice(HALF + rows.start, HALF + rows.stop), cols] = low
    for w in range(2):
        window = slice(128 * w, 128 * w + 256)
        out = None
        for d in range(2):
            both = dot(rho[d, :, window], wide_high[w, d])
            term = folded(both) + dot(rho[d, :HALF, window], wide_low[w, d])
            out = term if out is None else out + term
        for c in range(6):
            for i in range(4):
                y = 8 * c + 4 * w + i
                za[PITCH * y : PITCH * y + NG, :] = out[48 * c : 48 * c + 48, 128 * i : 128 * i + 128]

    def planes(ref, k):
        return jnp.concatenate([ref[PITCH * i : PITCH * i + NG, :] for i in (k, k + 1)], 1)

    def across(ref, k):
        return jnp.concatenate([ref[pl.ds(i, NG, stride=PITCH), :] for i in (k, k + 1)], 1)

    def put(ref, k, both):
        for e in range(2):
            ref[PITCH * (k + e) : PITCH * (k + e) + NG, :] = both[:, 128 * e : 128 * e + 128]

    for y in range(0, NG, 2):
        put(zb, y, left_mul(left_ref[0], planes(za, y)))
    for k in range(0, NG, 2):
        both = left_mul(left_ref[1], across(zb, k)) * jnp.concatenate([coulomb[k], coulomb[k + 1]], 1)
        put(za, k, left_mul(left_ref[2], both))
    for y in range(0, NG, 2):
        both = left_mul(left_ref[3], across(za, y))
        for e in range(2):
            c, w, i = (y + e) // 8, ((y + e) % 8) // 4, (y + e) % 4
            high, low = split(both[:, 128 * e : 128 * e + 128])
            solved[w, 48 * c : 48 * c + 48, 128 * i : 128 * i + 128] = high
            solved[w, HALF + 48 * c : HALF + 48 * c + 48, 128 * i : 128 * i + 128] = low
    thirds = []
    for d in range(2):
        a, b = [
            folded(dot_t(solved[w], wide_high[w, d])) + dot_t(solved[w, :HALF], wide_low[w, d]) for w in range(2)
        ]
        thirds.append((a[:, :128], a[:, 128:] + b[:, :128], b[:, 128:]))
    for c in range(COLS):
        rows, _ = place(c)
        out = thirds[0][c % 3][rows] * partner(0, c)
        out = out + thirds[1][c % 3][rows] * partner(1, c)
        for p in range(PLANES):
            out_ref[pl.ds(COLS * p + c, SLABS, stride=ROWS), :] = out[16 * p : 16 * p + 16]
    for r in range(USED, ROWS):
        out_ref[pl.ds(r, SLABS, stride=ROWS), :] = jnp.zeros((SLABS, 128), f32)


def partial_exchange(own, pair, made):
    big = pltpu.VMEM((NG * PITCH, 128), f32)
    rho, solved = pltpu.VMEM((2, 2 * HALF, 384), bf16), pltpu.VMEM((2, 2 * HALF, 512), bf16)
    return pl.pallas_call(
        exchange_kernel,
        out_shape=jax.ShapeDtypeStruct((SLABS * ROWS, 128), f32),
        scratch_shapes=[rho, big, big, solved],
        name="exchange",
        compiler_params=LARGE,
    )(own, pair, jnp.asarray(LEFTS), *made)


def prepare_kernel(slab_ref, copies_ref, tile_ref):
    tile_ref[USED:ROWS, :] = jnp.zeros((ROWS - USED, 128), f32)
    for p in range(PLANES):
        for c in range(COLS):
            r = COLS * p + c
            tile_ref[r : r + 1, :] = slab_ref[p, :, 128 * c : 128 * c + 128]
    tile = tile_ref[...]
    for k in range(CHIPS):
        copies_ref[k] = tile


def prepare(slab):
    return pl.pallas_call(
        prepare_kernel,
        out_shape=jax.ShapeDtypeStruct((CHIPS, ROWS, 128), f32),
        scratch_shapes=[pltpu.VMEM((ROWS, 128), f32)],
        name="prepare",
        compiler_params=SMALL,
    )(slab)


def role_of(xl):
    xh = lax.axis_index("xh")
    return xl + xh - 2 * xl * xh


def join_kernel(chips_ref, out_ref):
    tile = chips_ref[role_of(lax.axis_index("xl")) * 8 + lax.axis_index(("z4", "z2", "z1"))]
    for k in range(SLABS):
        out_ref[k, :ROWS, :] = tile
        out_ref[k, ROWS:, :] = chips_ref[k]


def join(chips):
    return pl.pallas_call(
        join_kernel,
        out_shape=jax.ShapeDtypeStruct((SLABS, 2 * ROWS, 128), f32),
        name="join",
        compiler_params=SMALL,
    )(chips)


def column_kernel(share_ref, orbital_ref, field_ref, copies_ref):
    field = jnp.sum(share_ref[...], axis=0)
    field_ref[...] = field
    sums = [
        jnp.sum(field * orbital_ref[ROWS * k : ROWS * k + ROWS, :], axis=0, keepdims=True) for k in range(BANDS)
    ]
    high, low = split(jnp.concatenate(sums + [jnp.zeros((128 - BANDS, 128), f32)], 0))
    ones = jnp.ones((8, 128), bf16)
    line = dot_t(ones, high) + dot_t(ones, low)
    for k in range(SLABS):
        copies_ref[k] = line


def column_part(shares, orbitals):
    field = jax.ShapeDtypeStruct((ROWS, 128), f32)
    copies = jax.ShapeDtypeStruct((SLABS, 8, 128), f32)
    return pl.pallas_call(column_kernel, out_shape=(field, copies), name="column", compiler_params=SMALL)(
        shares, orbitals
    )


def attach_kernel(field_ref, parts_ref, copies_ref):
    column = jnp.sum(parts_ref[...], axis=0)[:1]
    row = lax.broadcasted_iota(jnp.int32, (ROWS, 128), 0)
    tile = jnp.where(row == USED, column, field_ref[...])
    for k in range(CHIPS):
        copies_ref[k] = tile


def attach(field, parts):
    copies = jax.ShapeDtypeStruct((CHIPS, ROWS, 128), f32)
    return pl.pallas_call(attach_kernel, out_shape=copies, name="attach", compiler_params=SMALL)(field, parts)


BLOCK = 8


def place_of(band):
    return (band % 2) * CHIPS + band // 2


def finish_kernel(field_ref, out_ref, flat):
    mine = lax.axis_index(CORE + PAIR)
    starts = [ROWS * (CHIPS * core + 8 * role_of(xl)) for core in range(2) for xl in range(2)]
    matrix = jnp.concatenate([field_ref[pl.ds(start + USED, 8, stride=ROWS), :] for start in starts], 0)
    matrix = matrix[:, :BANDS]
    definite = (matrix + matrix.T) * (-0.5 / float(NG**3))
    row = lax.broadcasted_iota(jnp.int32, (BANDS, 2 * BANDS), 0)
    lane = lax.broadcasted_iota(jnp.int32, (BANDS, 2 * BANDS), 1)
    order = 2 * (row % CHIPS) + row // CHIPS
    unit = jnp.where(row[:, :BANDS] == lane[:, :BANDS], 1.0, 0.0).astype(f32)
    state = jnp.concatenate([definite, unit], 1)
    for first in range(0, BANDS, BLOCK):
        at = [place_of(first + i) for i in range(BLOCK)]
        columns = [jnp.broadcast_to(state[:, a : a + 1], (BANDS, 2 * BANDS)) for a in at]
        pivots = [state[a : a + 1, :] for a in at]
        for i in range(BLOCK):
            factor = jnp.where(order > first + i, columns[i] / columns[i][at[i] : at[i] + 1, :], 0.0)
            for j in range(i + 1, BLOCK):
                columns[j] = columns[j] - factor * columns[j][at[i] : at[i] + 1, :]
                pivots[j] = pivots[j] - factor[at[j] : at[j] + 1, :] * pivots[i]
            state = state - factor * pivots[i]
    picked = jnp.sum(jnp.where(row == mine, state, 0.0), axis=0, keepdims=True)
    pivot = jnp.sum(jnp.where(lane[:1] == mine, picked, 0.0), axis=1, keepdims=True)
    weights = picked * lax.rsqrt(pivot)
    total = None
    for k in range(BANDS):
        weight = weights[:, BANDS + k : BANDS + k + 1]
        start = pl.multiple_of(starts[k // 8] + ROWS * (k % 8), 8)
        term = weight * field_ref[pl.ds(start, ROWS), :]
        total = term if total is None else total + term
    flat[...] = total
    for p in range(PLANES):
        for c in range(COLS):
            r = COLS * p + c
            out_ref[p, :, 128 * c : 128 * c + 128] = flat[r : r + 1, :]


def finish(fields):
    return pl.pallas_call(
        finish_kernel,
        out_shape=jax.ShapeDtypeStruct((PLANES, 1, NG * NG), f32),
        scratch_shapes=[pltpu.VMEM((ROWS, 128), f32)],
        name="finish",
        compiler_params=SMALL,
    )(fields)


def exchange_tiles(tiles, axis):
    return lax.all_to_all(tiles, axis, 0, 0, tiled=True)


def exchange_roles(tiles):
    return lax.all_to_all(tiles, CROSS, 0, 0, axis_index_groups=ROLES, tiled=True)


def both_cores(chips):
    return lax.all_gather(chips, CORE, axis=0, tiled=False).reshape(-1, 128)


def per_device(orbitals):
    copies = prepare(jnp.transpose(orbitals, (1, 0, 2)))
    made = tables(jnp.asarray(LAST_HIGH), jnp.asarray(LAST_LOW))
    chips = exchange_tiles(copies, PAIR)
    whole, others = lax.optimization_barrier((exchange_roles(join(chips)), both_cores(chips)))
    pair = both_cores(whole[:, ROWS:])
    partial = partial_exchange(whole.reshape(SLABS * 2 * ROWS, 128), pair, made)
    shares = exchange_roles(partial.reshape(SLABS, ROWS, 128))
    field, lines = column_part(shares, others)
    parts = exchange_roles(lines)
    fields = both_cores(exchange_tiles(attach(field, parts), PAIR))
    return jnp.transpose(finish(fields), (1, 0, 2))


def solution(mesh):
    parted = Mesh(mesh.devices.reshape((2,) * 9), BAND + GRID)
    spec = P(BAND, GRID, None)
    return jax.shard_map(per_device, mesh=parted, in_specs=(spec,), out_specs=spec, check_vma=False)
```

```python
import math

import jax
import jax.numpy as jnp
import numpy as np
from jax import lax
from jax.experimental import pallas as pl
from jax.experimental.pallas import tpu as pltpu
from jax.sharding import Mesh, PartitionSpec as P

NG = 48
BANDS = 32
COULOMB = 50.0
SLABS = 16
PLANES = NG // SLABS
COLS = NG * NG // 128
ROWS = 56
USED = PLANES * COLS
CHIPS = BANDS // 2
PAIR, CORE, GRID = ("xl", "z4", "z2", "z1"), ("c",), ("xh", "y4", "y2", "y1")
BAND = PAIR + CORE
CROSS = ("xl",) + GRID
ROLES = [[(q ^ h) * 16 + h * 8 + y for h in range(2) for y in range(8)] for q in range(2)]
PITCH = 56
f32, bf16 = jnp.float32, jnp.bfloat16
SMALL = pltpu.CompilerParams(vmem_limit_bytes=12 << 20)
LARGE = pltpu.CompilerParams(vmem_limit_bytes=24 << 20)


def real_basis():
    half = NG // 2
    freq = np.concatenate([np.arange(half + 1), np.arange(1, half)])
    turn = 2.0 * np.pi * ((freq[:, None] * np.arange(NG)[None, :]) % NG) / NG
    wave = np.where(np.arange(NG)[:, None] <= half, np.cos(turn), np.sin(turn))
    norm = np.where((np.arange(NG) == 0) | (np.arange(NG) == half), 1.0, 2.0) / NG
    return wave * np.sqrt(norm)[:, None], freq.astype(np.float64) ** 2


def halves(matrix):
    high = matrix.astype(np.float32).astype(bf16)
    low = (matrix - high.astype(np.float64)).astype(np.float32).astype(bf16)
    return high, low


def from_left(matrix):
    high, low = halves(matrix)
    return np.concatenate([high, high, low], 1)


BASIS, SQUARES = real_basis()
BASIS_X = BASIS[:, [PLANES * (r % SLABS) + r // SLABS for r in range(NG)]]
LEFTS = np.stack([from_left(m) for m in (BASIS_X, BASIS, BASIS.T, BASIS_X.T)])


def last_edge():
    wide = np.zeros((2, NG, 128))
    wide[0, :, :NG] = BASIS.T
    wide[1, :, 64 : 64 + NG] = BASIS.T
    return halves(wide)


LAST_HIGH, LAST_LOW = last_edge()


def split(x):
    high = x.astype(bf16)
    return high, (x - high.astype(f32)).astype(bf16)


def dot(a, b):
    return jnp.dot(a, b, preferred_element_type=f32)


def dot_t(a, b):
    return lax.dot_general(a, b, (((1,), (1,)), ((), ())), preferred_element_type=f32)


def left_mul(matrix, x):
    high, low = split(x)
    return dot(matrix, jnp.concatenate([high, low, high], 0))


def tables_kernel(high_ref, low_ref, wide_high, wide_low, coulomb):
    wide_high[...] = jnp.zeros_like(wide_high)
    wide_low[...] = jnp.zeros_like(wide_low)
    for w in range(2):
        for d in range(2):
            for i in range(4):
                rows = slice(48 * i + 64 * w, 48 * i + 64 * w + 48)
                cols = slice(128 * i, 128 * i + 128)
                wide_high[w, d, rows, cols] = high_ref[d]
                wide_low[w, d, rows, cols] = low_ref[d]

    def square(i):
        freq = jnp.where(i <= NG // 2, i, i - NG // 2).astype(f32)
        return freq * freq

    middle = lax.broadcasted_iota(jnp.int32, (NG, 128), 0)
    lane = lax.broadcasted_iota(jnp.int32, (NG, 128), 1)
    last = jnp.minimum(jnp.where(lane >= 64, lane - 64, lane), NG - 1)
    rest = square(middle) + square(last)
    for k in range(NG):
        total = rest + float(SQUARES[k])
        coulomb[k] = jnp.where(total > 0.0, -COULOMB / jnp.maximum(total, 1.0), 0.0)


def tables(last_high, last_low):
    wide = jax.ShapeDtypeStruct((2, 2, 256, 512), bf16)
    return pl.pallas_call(
        tables_kernel,
        out_shape=(wide, wide, jax.ShapeDtypeStruct((NG, NG, 128), f32)),
        name="tables",
        compiler_params=SMALL,
    )(last_high, last_low)


HALF = 6 * NG


def folded(x):
    return x[:HALF] + x[HALF:]


def exchange_kernel(
    own_ref, pair_ref, left_ref, wide_high, wide_low, coulomb, out_ref, rho, za, zb, solved
):
    def column(ref, first, c, step=ROWS):
        return jnp.concatenate(
            [ref[pl.ds(first + COLS * p + c, SLABS, stride=step), :] for p in range(PLANES)], 0
        )

    def partner(d, c):
        return column(pair_ref, d * SLABS * ROWS, c)

    def place(c):
        return slice(48 * (c // 3), 48 * (c // 3) + 48), slice(128 * (c % 3), 128 * (c % 3) + 128)

    for c in range(COLS):
        own = column(own_ref, 0, c, 2 * ROWS)
        rows, cols = place(c)
        for d in range(2):
            high, low = split(own * partner(d, c))
            rho[d, rows, cols] = high
            rho[d, slice(HALF + rows.start, HALF + rows.stop), cols] = low
    for w in range(2):
        window = slice(128 * w, 128 * w + 256)
        out = None
        for d in range(2):
            both = dot(rho[d, :, window], wide_high[w, d])
            term = folded(both) + dot(rho[d, :HALF, window], wide_low[w, d])
            out = term if out is None else out + term
        for c in range(6):
            for i in range(4):
                y = 8 * c + 4 * w + i
                za[PITCH * y : PITCH * y + NG, :] = out[48 * c : 48 * c + 48, 128 * i : 128 * i + 128]

    def planes(ref, k):
        return jnp.concatenate([ref[PITCH * i : PITCH * i + NG, :] for i in (k, k + 1)], 1)

    def across(ref, k):
        return jnp.concatenate([ref[pl.ds(i, NG, stride=PITCH), :] for i in (k, k + 1)], 1)

    def put(ref, k, both):
        for e in range(2):
            ref[PITCH * (k + e) : PITCH * (k + e) + NG, :] = both[:, 128 * e : 128 * e + 128]

    for y in range(0, NG, 2):
        put(zb, y, left_mul(left_ref[0], planes(za, y)))
    for k in range(0, NG, 2):
        both = left_mul(left_ref[1], across(zb, k)) * jnp.concatenate([coulomb[k], coulomb[k + 1]], 1)
        put(za, k, left_mul(left_ref[2], both))
    for y in range(0, NG, 2):
        both = left_mul(left_ref[3], across(za, y))
        for e in range(2):
            c, w, i = (y + e) // 8, ((y + e) % 8) // 4, (y + e) % 4
            high, low = split(both[:, 128 * e : 128 * e + 128])
            solved[w, 48 * c : 48 * c + 48, 128 * i : 128 * i + 128] = high
            solved[w, HALF + 48 * c : HALF + 48 * c + 48, 128 * i : 128 * i + 128] = low
    thirds = []
    for d in range(2):
        a, b = [
            folded(dot_t(solved[w], wide_high[w, d])) + dot_t(solved[w, :HALF], wide_low[w, d]) for w in range(2)
        ]
        thirds.append((a[:, :128], a[:, 128:] + b[:, :128], b[:, 128:]))
    for c in range(COLS):
        rows, _ = place(c)
        out = thirds[0][c % 3][rows] * partner(0, c)
        out = out + thirds[1][c % 3][rows] * partner(1, c)
        for p in range(PLANES):
            out_ref[pl.ds(COLS * p + c, SLABS, stride=ROWS), :] = out[16 * p : 16 * p + 16]
    for r in range(USED, ROWS):
        out_ref[pl.ds(r, SLABS, stride=ROWS), :] = jnp.zeros((SLABS, 128), f32)


def partial_exchange(own, pair, made):
    big = pltpu.VMEM((NG * PITCH, 128), f32)
    rho, solved = pltpu.VMEM((2, 2 * HALF, 384), bf16), pltpu.VMEM((2, 2 * HALF, 512), bf16)
    return pl.pallas_call(
        exchange_kernel,
        out_shape=jax.ShapeDtypeStruct((SLABS * ROWS, 128), f32),
        scratch_shapes=[rho, big, big, solved],
        name="exchange",
        compiler_params=LARGE,
    )(own, pair, jnp.asarray(LEFTS), *made)


def prepare_kernel(slab_ref, copies_ref, tile_ref):
    tile_ref[USED:ROWS, :] = jnp.zeros((ROWS - USED, 128), f32)
    for p in range(PLANES):
        for c in range(COLS):
            r = COLS * p + c
            tile_ref[r : r + 1, :] = slab_ref[p, :, 128 * c : 128 * c + 128]
    tile = tile_ref[...]
    for k in range(CHIPS):
        copies_ref[k] = tile


def prepare(slab):
    return pl.pallas_call(
        prepare_kernel,
        out_shape=jax.ShapeDtypeStruct((CHIPS, ROWS, 128), f32),
        scratch_shapes=[pltpu.VMEM((ROWS, 128), f32)],
        name="prepare",
        compiler_params=SMALL,
    )(slab)


def role_of(xl):
    xh = lax.axis_index("xh")
    return xl + xh - 2 * xl * xh


def join_kernel(chips_ref, out_ref):
    tile = chips_ref[role_of(lax.axis_index("xl")) * 8 + lax.axis_index(("z4", "z2", "z1"))]
    for k in range(SLABS):
        out_ref[k, :ROWS, :] = tile
        out_ref[k, ROWS:, :] = chips_ref[k]


def join(chips):
    return pl.pallas_call(
        join_kernel,
        out_shape=jax.ShapeDtypeStruct((SLABS, 2 * ROWS, 128), f32),
        name="join",
        compiler_params=SMALL,
    )(chips)


def column_kernel(share_ref, orbital_ref, field_ref, copies_ref):
    field = jnp.sum(share_ref[...], axis=0)
    field_ref[...] = field
    sums = [
        jnp.sum(field * orbital_ref[ROWS * k : ROWS * k + ROWS, :], axis=0, keepdims=True) for k in range(BANDS)
    ]
    high, low = split(jnp.concatenate(sums + [jnp.zeros((128 - BANDS, 128), f32)], 0))
    ones = jnp.ones((8, 128), bf16)
    line = dot_t(ones, high) + dot_t(ones, low)
    for k in range(SLABS):
        copies_ref[k] = line


def column_part(shares, orbitals):
    field = jax.ShapeDtypeStruct((ROWS, 128), f32)
    copies = jax.ShapeDtypeStruct((SLABS, 8, 128), f32)
    return pl.pallas_call(column_kernel, out_shape=(field, copies), name="column", compiler_params=SMALL)(
        shares, orbitals
    )


def attach_kernel(field_ref, parts_ref, copies_ref):
    column = jnp.sum(parts_ref[...], axis=0)[:1]
    row = lax.broadcasted_iota(jnp.int32, (ROWS, 128), 0)
    tile = jnp.where(row == USED, column, field_ref[...])
    for k in range(CHIPS):
        copies_ref[k] = tile


def attach(field, parts):
    copies = jax.ShapeDtypeStruct((CHIPS, ROWS, 128), f32)
    return pl.pallas_call(attach_kernel, out_shape=copies, name="attach", compiler_params=SMALL)(field, parts)


BLOCK = 16


def place_of(band):
    return (band % 2) * CHIPS + band // 2


def finish_kernel(field_ref, out_ref, flat):
    mine = lax.axis_index(CORE + PAIR)
    starts = [ROWS * (CHIPS * core + 8 * role_of(xl)) for core in range(2) for xl in range(2)]
    matrix = jnp.concatenate([field_ref[pl.ds(start + USED, 8, stride=ROWS), :] for start in starts], 0)
    matrix = matrix[:, :BANDS]
    definite = (matrix + matrix.T) * (-0.5 / float(NG**3))
    row = lax.broadcasted_iota(jnp.int32, (BANDS, 2 * BANDS), 0)
    lane = lax.broadcasted_iota(jnp.int32, (BANDS, 2 * BANDS), 1)
    order = 2 * (row % CHIPS) + row // CHIPS
    unit = jnp.where(row[:, :BANDS] == lane[:, :BANDS], 1.0, 0.0).astype(f32)
    state = jnp.concatenate([definite, unit], 1)
    for first in range(0, BANDS, BLOCK):
        at = [place_of(first + i) for i in range(BLOCK)]
        columns = [jnp.broadcast_to(state[:, a : a + 1], (BANDS, 2 * BANDS)) for a in at]
        pivots = [state[a : a + 1, :] for a in at]
        for i in range(BLOCK):
            inverse = 1.0 / columns[i][at[i] : at[i] + 1, :]
            factor = jnp.where(order > first + i, columns[i] * inverse, 0.0)
            for j in range(i + 1, BLOCK):
                columns[j] = columns[j] - factor * columns[j][at[i] : at[i] + 1, :]
                pivots[j] = pivots[j] - factor[at[j] : at[j] + 1, :] * pivots[i]
            state = state - factor * pivots[i]
    picked = jnp.sum(jnp.where(row == mine, state, 0.0), axis=0, keepdims=True)
    pivot = jnp.sum(jnp.where(lane[:1] == mine, picked, 0.0), axis=1, keepdims=True)
    weights = picked * lax.rsqrt(pivot)
    total = None
    for k in range(BANDS):
        weight = weights[:, BANDS + k : BANDS + k + 1]
        start = pl.multiple_of(starts[k // 8] + ROWS * (k % 8), 8)
        term = weight * field_ref[pl.ds(start, ROWS), :]
        total = term if total is None else total + term
    flat[...] = total
    for p in range(PLANES):
        for c in range(COLS):
            r = COLS * p + c
            out_ref[p, :, 128 * c : 128 * c + 128] = flat[r : r + 1, :]


def finish(fields):
    return pl.pallas_call(
        finish_kernel,
        out_shape=jax.ShapeDtypeStruct((PLANES, 1, NG * NG), f32),
        scratch_shapes=[pltpu.VMEM((ROWS, 128), f32)],
        name="finish",
        compiler_params=SMALL,
    )(fields)


def exchange_tiles(tiles, axis):
    return lax.all_to_all(tiles, axis, 0, 0, tiled=True)


def exchange_roles(tiles):
    return lax.all_to_all(tiles, CROSS, 0, 0, axis_index_groups=ROLES, tiled=True)


def both_cores(chips):
    return lax.all_gather(chips, CORE, axis=0, tiled=False).reshape(-1, 128)


def per_device(orbitals):
    copies = prepare(jnp.transpose(orbitals, (1, 0, 2)))
    made = tables(jnp.asarray(LAST_HIGH), jnp.asarray(LAST_LOW))
    chips = exchange_tiles(copies, PAIR)
    whole, others = lax.optimization_barrier((exchange_roles(join(chips)), both_cores(chips)))
    pair = both_cores(whole[:, ROWS:])
    partial = partial_exchange(whole.reshape(SLABS * 2 * ROWS, 128), pair, made)
    shares = exchange_roles(partial.reshape(SLABS, ROWS, 128))
    field, lines = column_part(shares, others)
    parts = exchange_roles(lines)
    fields = both_cores(exchange_tiles(attach(field, parts), PAIR))
    return jnp.transpose(finish(fields), (1, 0, 2))


def solution(mesh):
    parted = Mesh(mesh.devices.reshape((2,) * 9), BAND + GRID)
    spec = P(BAND, GRID, None)
    return jax.shard_map(per_device, mesh=parted, in_specs=(spec,), out_specs=spec, check_vma=False)
```

```python
import math

import jax
import jax.numpy as jnp
import numpy as np
from jax import lax
from jax.experimental import pallas as pl
from jax.experimental.pallas import tpu as pltpu
from jax.sharding import Mesh, PartitionSpec as P

NG = 48
BANDS = 32
COULOMB = 50.0
SLABS = 16
PLANES = NG // SLABS
COLS = NG * NG // 128
ROWS = 56
USED = PLANES * COLS
CHIPS = BANDS // 2
PAIR, CORE, GRID = ("xl", "z4", "z2", "z1"), ("c",), ("xh", "y4", "y2", "y1")
BAND = PAIR + CORE
CROSS = ("xl",) + GRID
ROLES = [[(q ^ h) * 16 + h * 8 + y for h in range(2) for y in range(8)] for q in range(2)]
PITCH = 56
f32, bf16 = jnp.float32, jnp.bfloat16
SMALL = pltpu.CompilerParams(vmem_limit_bytes=12 << 20)
LARGE = pltpu.CompilerParams(vmem_limit_bytes=24 << 20)


def real_basis():
    half = NG // 2
    freq = np.concatenate([np.arange(half + 1), np.arange(1, half)])
    turn = 2.0 * np.pi * ((freq[:, None] * np.arange(NG)[None, :]) % NG) / NG
    wave = np.where(np.arange(NG)[:, None] <= half, np.cos(turn), np.sin(turn))
    norm = np.where((np.arange(NG) == 0) | (np.arange(NG) == half), 1.0, 2.0) / NG
    return wave * np.sqrt(norm)[:, None], freq.astype(np.float64) ** 2


def halves(matrix):
    high = matrix.astype(np.float32).astype(bf16)
    low = (matrix - high.astype(np.float64)).astype(np.float32).astype(bf16)
    return high, low


def from_left(matrix):
    high, low = halves(matrix)
    return np.concatenate([high, high, low], 1)


BASIS, SQUARES = real_basis()
BASIS_X = BASIS[:, [PLANES * (r % SLABS) + r // SLABS for r in range(NG)]]
LEFTS = np.stack([from_left(m) for m in (BASIS_X, BASIS, BASIS.T, BASIS_X.T)])


def last_edge():
    wide = np.zeros((2, NG, 128))
    wide[0, :, :NG] = BASIS.T
    wide[1, :, 64 : 64 + NG] = BASIS.T
    return halves(wide)


LAST_HIGH, LAST_LOW = last_edge()


def split(x):
    high = x.astype(bf16)
    return high, (x - high.astype(f32)).astype(bf16)


def dot(a, b):
    return jnp.dot(a, b, preferred_element_type=f32)


def dot_t(a, b):
    return lax.dot_general(a, b, (((1,), (1,)), ((), ())), preferred_element_type=f32)


def left_mul(matrix, x):
    high, low = split(x)
    return dot(matrix, jnp.concatenate([high, low, high], 0))


def tables_kernel(high_ref, low_ref, wide_high, wide_low, coulomb):
    wide_high[...] = jnp.zeros_like(wide_high)
    wide_low[...] = jnp.zeros_like(wide_low)
    for w in range(2):
        for d in range(2):
            for i in range(4):
                rows = slice(48 * i + 64 * w, 48 * i + 64 * w + 48)
                cols = slice(128 * i, 128 * i + 128)
                wide_high[w, d, rows, cols] = high_ref[d]
                wide_low[w, d, rows, cols] = low_ref[d]

    def square(i):
        freq = jnp.where(i <= NG // 2, i, i - NG // 2).astype(f32)
        return freq * freq

    middle = lax.broadcasted_iota(jnp.int32, (NG, 128), 0)
    lane = lax.broadcasted_iota(jnp.int32, (NG, 128), 1)
    last = jnp.minimum(jnp.where(lane >= 64, lane - 64, lane), NG - 1)
    rest = square(middle) + square(last)
    for k in range(NG):
        total = rest + float(SQUARES[k])
        coulomb[k] = jnp.where(total > 0.0, -COULOMB / jnp.maximum(total, 1.0), 0.0)


def tables(last_high, last_low):
    wide = jax.ShapeDtypeStruct((2, 2, 256, 512), bf16)
    return pl.pallas_call(
        tables_kernel,
        out_shape=(wide, wide, jax.ShapeDtypeStruct((NG, NG, 128), f32)),
        name="tables",
        compiler_params=SMALL,
    )(last_high, last_low)


HALF = 6 * NG


def folded(x):
    return x[:HALF] + x[HALF:]


def exchange_kernel(
    own_ref, pair_ref, left_ref, wide_high, wide_low, coulomb, out_ref, rho, za, zb, solved
):
    def column(ref, first, c, step=ROWS):
        return jnp.concatenate(
            [ref[pl.ds(first + COLS * p + c, SLABS, stride=step), :] for p in range(PLANES)], 0
        )

    def partner(d, c):
        return column(pair_ref, d * SLABS * ROWS, c)

    def place(c):
        return slice(48 * (c // 3), 48 * (c // 3) + 48), slice(128 * (c % 3), 128 * (c % 3) + 128)

    for c in range(COLS):
        own = column(own_ref, 0, c, 2 * ROWS)
        rows, cols = place(c)
        for d in range(2):
            high, low = split(own * partner(d, c))
            rho[d, rows, cols] = high
            rho[d, slice(HALF + rows.start, HALF + rows.stop), cols] = low
    for w in range(2):
        window = slice(128 * w, 128 * w + 256)
        out = None
        for d in range(2):
            both = dot(rho[d, :, window], wide_high[w, d])
            term = folded(both) + dot(rho[d, :HALF, window], wide_low[w, d])
            out = term if out is None else out + term
        for c in range(6):
            for i in range(4):
                y = 8 * c + 4 * w + i
                za[PITCH * y : PITCH * y + NG, :] = out[48 * c : 48 * c + 48, 128 * i : 128 * i + 128]

    def planes(ref, k):
        return jnp.concatenate([ref[PITCH * i : PITCH * i + NG, :] for i in (k, k + 1)], 1)

    def across(ref, k):
        return jnp.concatenate([ref[pl.ds(i, NG, stride=PITCH), :] for i in (k, k + 1)], 1)

    def put(ref, k, both):
        for e in range(2):
            ref[PITCH * (k + e) : PITCH * (k + e) + NG, :] = both[:, 128 * e : 128 * e + 128]

    for y in range(0, NG, 2):
        put(zb, y, left_mul(left_ref[0], planes(za, y)))
    for k in range(0, NG, 2):
        both = left_mul(left_ref[1], across(zb, k)) * jnp.concatenate([coulomb[k], coulomb[k + 1]], 1)
        put(za, k, left_mul(left_ref[2], both))
    for y in range(0, NG, 2):
        both = left_mul(left_ref[3], across(za, y))
        for e in range(2):
            c, w, i = (y + e) // 8, ((y + e) % 8) // 4, (y + e) % 4
            high, low = split(both[:, 128 * e : 128 * e + 128])
            solved[w, 48 * c : 48 * c + 48, 128 * i : 128 * i + 128] = high
            solved[w, HALF + 48 * c : HALF + 48 * c + 48, 128 * i : 128 * i + 128] = low
    thirds = []
    for d in range(2):
        a, b = [
            folded(dot_t(solved[w], wide_high[w, d])) + dot_t(solved[w, :HALF], wide_low[w, d]) for w in range(2)
        ]
        thirds.append((a[:, :128], a[:, 128:] + b[:, :128], b[:, 128:]))
    for c in range(COLS):
        rows, _ = place(c)
        out = thirds[0][c % 3][rows] * partner(0, c)
        out = out + thirds[1][c % 3][rows] * partner(1, c)
        for p in range(PLANES):
            out_ref[pl.ds(COLS * p + c, SLABS, stride=ROWS), :] = out[16 * p : 16 * p + 16]
    for r in range(USED, ROWS):
        out_ref[pl.ds(r, SLABS, stride=ROWS), :] = jnp.zeros((SLABS, 128), f32)


def partial_exchange(own, pair, made):
    big = pltpu.VMEM((NG * PITCH, 128), f32)
    rho, solved = pltpu.VMEM((2, 2 * HALF, 384), bf16), pltpu.VMEM((2, 2 * HALF, 512), bf16)
    return pl.pallas_call(
        exchange_kernel,
        out_shape=jax.ShapeDtypeStruct((SLABS * ROWS, 128), f32),
        scratch_shapes=[rho, big, big, solved],
        name="exchange",
        compiler_params=LARGE,
    )(own, pair, jnp.asarray(LEFTS), *made)


def prepare_kernel(slab_ref, copies_ref, tile_ref):
    tile_ref[USED:ROWS, :] = jnp.zeros((ROWS - USED, 128), f32)
    for p in range(PLANES):
        for c in range(COLS):
            r = COLS * p + c
            tile_ref[r : r + 1, :] = slab_ref[p, :, 128 * c : 128 * c + 128]
    tile = tile_ref[...]
    for k in range(CHIPS):
        copies_ref[k] = tile


def prepare(slab):
    return pl.pallas_call(
        prepare_kernel,
        out_shape=jax.ShapeDtypeStruct((CHIPS, ROWS, 128), f32),
        scratch_shapes=[pltpu.VMEM((ROWS, 128), f32)],
        name="prepare",
        compiler_params=SMALL,
    )(slab)


def role_of(xl):
    xh = lax.axis_index("xh")
    return xl + xh - 2 * xl * xh


def join_kernel(chips_ref, out_ref):
    tile = chips_ref[role_of(lax.axis_index("xl")) * 8 + lax.axis_index(("z4", "z2", "z1"))]
    for k in range(SLABS):
        out_ref[k, :ROWS, :] = tile
        out_ref[k, ROWS:, :] = chips_ref[k]


def join(chips):
    return pl.pallas_call(
        join_kernel,
        out_shape=jax.ShapeDtypeStruct((SLABS, 2 * ROWS, 128), f32),
        name="join",
        compiler_params=SMALL,
    )(chips)


def column_kernel(share_ref, orbital_ref, field_ref, copies_ref):
    field = jnp.sum(share_ref[...], axis=0)
    field_ref[...] = field
    sums = [
        jnp.sum(field * orbital_ref[ROWS * k : ROWS * k + ROWS, :], axis=0, keepdims=True) for k in range(BANDS)
    ]
    high, low = split(jnp.concatenate(sums + [jnp.zeros((128 - BANDS, 128), f32)], 0))
    ones = jnp.ones((8, 128), bf16)
    line = (dot_t(ones, high) + dot_t(ones, low))[:1]
    for k in range(SLABS):
        copies_ref[k] = line


def column_part(shares, orbitals):
    field = jax.ShapeDtypeStruct((ROWS, 128), f32)
    copies = jax.ShapeDtypeStruct((SLABS, 1, 128), f32)
    return pl.pallas_call(column_kernel, out_shape=(field, copies), name="column", compiler_params=SMALL)(
        shares, orbitals
    )


def attach_kernel(field_ref, parts_ref, copies_ref):
    column = sum(parts_ref[k] for k in range(SLABS))
    row = lax.broadcasted_iota(jnp.int32, (ROWS, 128), 0)
    tile = jnp.where(row == USED, column, field_ref[...])
    for k in range(CHIPS):
        copies_ref[k] = tile


def attach(field, parts):
    copies = jax.ShapeDtypeStruct((CHIPS, ROWS, 128), f32)
    return pl.pallas_call(attach_kernel, out_shape=copies, name="attach", compiler_params=SMALL)(field, parts)


BLOCK = 8


def place_of(band):
    return (band % 2) * CHIPS + band // 2


def finish_kernel(field_ref, out_ref, flat):
    mine = lax.axis_index(CORE + PAIR)
    starts = [ROWS * (CHIPS * core + 8 * role_of(xl)) for core in range(2) for xl in range(2)]
    matrix = jnp.concatenate([field_ref[pl.ds(start + USED, 8, stride=ROWS), :] for start in starts], 0)
    matrix = matrix[:, :BANDS]
    definite = (matrix + matrix.T) * (-0.5 / float(NG**3))
    row = lax.broadcasted_iota(jnp.int32, (BANDS, 2 * BANDS), 0)
    lane = lax.broadcasted_iota(jnp.int32, (BANDS, 2 * BANDS), 1)
    order = 2 * (row % CHIPS) + row // CHIPS
    unit = jnp.where(row[:, :BANDS] == lane[:, :BANDS], 1.0, 0.0).astype(f32)
    state = jnp.concatenate([definite, unit], 1)
    for first in range(0, BANDS, BLOCK):
        at = [place_of(first + i) for i in range(BLOCK)]
        columns = [jnp.broadcast_to(state[:, a : a + 1], (BANDS, 2 * BANDS)) for a in at]
        pivots = [state[a : a + 1, :] for a in at]
        for i in range(BLOCK):
            factor = jnp.where(order > first + i, columns[i] / columns[i][at[i] : at[i] + 1, :], 0.0)
            for j in range(i + 1, BLOCK):
                columns[j] = columns[j] - factor * columns[j][at[i] : at[i] + 1, :]
                pivots[j] = pivots[j] - factor[at[j] : at[j] + 1, :] * pivots[i]
            state = state - factor * pivots[i]
    picked = jnp.sum(jnp.where(row == mine, state, 0.0), axis=0, keepdims=True)
    pivot = jnp.sum(jnp.where(lane[:1] == mine, picked, 0.0), axis=1, keepdims=True)
    weights = picked * lax.rsqrt(pivot)
    total = None
    for k in range(BANDS):
        weight = weights[:, BANDS + k : BANDS + k + 1]
        start = pl.multiple_of(starts[k // 8] + ROWS * (k % 8), 8)
        term = weight * field_ref[pl.ds(start, ROWS), :]
        total = term if total is None else total + term
    flat[...] = total
    for p in range(PLANES):
        for c in range(COLS):
            r = COLS * p + c
            out_ref[p, :, 128 * c : 128 * c + 128] = flat[r : r + 1, :]


def finish(fields):
    return pl.pallas_call(
        finish_kernel,
        out_shape=jax.ShapeDtypeStruct((PLANES, 1, NG * NG), f32),
        scratch_shapes=[pltpu.VMEM((ROWS, 128), f32)],
        name="finish",
        compiler_params=SMALL,
    )(fields)


def exchange_tiles(tiles, axis):
    return lax.all_to_all(tiles, axis, 0, 0, tiled=True)


def exchange_roles(tiles):
    return lax.all_to_all(tiles, CROSS, 0, 0, axis_index_groups=ROLES, tiled=True)


def both_cores(chips):
    return lax.all_gather(chips, CORE, axis=0, tiled=False).reshape(-1, 128)


def per_device(orbitals):
    copies = prepare(jnp.transpose(orbitals, (1, 0, 2)))
    made = tables(jnp.asarray(LAST_HIGH), jnp.asarray(LAST_LOW))
    chips = exchange_tiles(copies, PAIR)
    whole, others = lax.optimization_barrier((exchange_roles(join(chips)), both_cores(chips)))
    pair = both_cores(whole[:, ROWS:])
    partial = partial_exchange(whole.reshape(SLABS * 2 * ROWS, 128), pair, made)
    shares = exchange_roles(partial.reshape(SLABS, ROWS, 128))
    field, lines = column_part(shares, others)
    parts = exchange_roles(lines)
    fields = both_cores(exchange_tiles(attach(field, parts), PAIR))
    return jnp.transpose(finish(fields), (1, 0, 2))


def solution(mesh):
    parted = Mesh(mesh.devices.reshape((2,) * 9), BAND + GRID)
    spec = P(BAND, GRID, None)
    return jax.shard_map(per_device, mesh=parted, in_specs=(spec,), out_specs=spec, check_vma=False)
```

```python
import math

import jax
import jax.numpy as jnp
import numpy as np
from jax import lax
from jax.experimental import pallas as pl
from jax.experimental.pallas import tpu as pltpu
from jax.sharding import Mesh, PartitionSpec as P

NG = 48
BANDS = 32
COULOMB = 50.0
SLABS = 16
PLANES = NG // SLABS
COLS = NG * NG // 128
ROWS = 56
USED = PLANES * COLS
CHIPS = BANDS // 2
PAIR, CORE, GRID = ("xl", "z4", "z2", "z1"), ("c",), ("xh", "y4", "y2", "y1")
BAND = PAIR + CORE
CROSS = ("xl",) + GRID
ROLES = [[(q ^ h) * 16 + h * 8 + y for h in range(2) for y in range(8)] for q in range(2)]
PITCH = 56
f32, bf16 = jnp.float32, jnp.bfloat16
SMALL = pltpu.CompilerParams(vmem_limit_bytes=12 << 20)
LARGE = pltpu.CompilerParams(vmem_limit_bytes=24 << 20)


def real_basis():
    half = NG // 2
    freq = np.concatenate([np.arange(half + 1), np.arange(1, half)])
    turn = 2.0 * np.pi * ((freq[:, None] * np.arange(NG)[None, :]) % NG) / NG
    wave = np.where(np.arange(NG)[:, None] <= half, np.cos(turn), np.sin(turn))
    norm = np.where((np.arange(NG) == 0) | (np.arange(NG) == half), 1.0, 2.0) / NG
    return wave * np.sqrt(norm)[:, None], freq.astype(np.float64) ** 2


def halves(matrix):
    high = matrix.astype(np.float32).astype(bf16)
    low = (matrix - high.astype(np.float64)).astype(np.float32).astype(bf16)
    return high, low


def from_left(matrix):
    high, low = halves(matrix)
    return np.concatenate([high, high, low], 1)


BASIS, SQUARES = real_basis()
BASIS_X = BASIS[:, [PLANES * (r % SLABS) + r // SLABS for r in range(NG)]]
LEFTS = np.stack([from_left(m) for m in (BASIS_X, BASIS, BASIS.T, BASIS_X.T)])


def last_edge():
    wide = np.zeros((2, NG, 128))
    wide[0, :, :NG] = BASIS.T
    wide[1, :, 64 : 64 + NG] = BASIS.T
    return halves(wide)


LAST_HIGH, LAST_LOW = last_edge()


def split(x):
    high = x.astype(bf16)
    return high, (x - high.astype(f32)).astype(bf16)


def dot(a, b):
    return jnp.dot(a, b, preferred_element_type=f32)


def dot_t(a, b):
    return lax.dot_general(a, b, (((1,), (1,)), ((), ())), preferred_element_type=f32)


def left_mul(matrix, x):
    high, low = split(x)
    return dot(matrix, jnp.concatenate([high, low, high], 0))


def tables_kernel(high_ref, low_ref, wide_high, wide_low, coulomb):
    wide_high[...] = jnp.zeros_like(wide_high)
    wide_low[...] = jnp.zeros_like(wide_low)
    for w in range(2):
        for d in range(2):
            for i in range(4):
                rows = slice(48 * i + 64 * w, 48 * i + 64 * w + 48)
                cols = slice(128 * i, 128 * i + 128)
                wide_high[w, d, rows, cols] = high_ref[d]
                wide_low[w, d, rows, cols] = low_ref[d]

    def square(i):
        freq = jnp.where(i <= NG // 2, i, i - NG // 2).astype(f32)
        return freq * freq

    middle = lax.broadcasted_iota(jnp.int32, (NG, 128), 0)
    lane = lax.broadcasted_iota(jnp.int32, (NG, 128), 1)
    last = jnp.minimum(jnp.where(lane >= 64, lane - 64, lane), NG - 1)
    rest = square(middle) + square(last)
    for k in range(NG):
        total = rest + float(SQUARES[k])
        coulomb[k] = jnp.where(total > 0.0, -COULOMB / jnp.maximum(total, 1.0), 0.0)


def tables(last_high, last_low):
    wide = jax.ShapeDtypeStruct((2, 2, 256, 512), bf16)
    return pl.pallas_call(
        tables_kernel,
        out_shape=(wide, wide, jax.ShapeDtypeStruct((NG, NG, 128), f32)),
        name="tables",
        compiler_params=SMALL,
    )(last_high, last_low)


HALF = 6 * NG


def folded(x):
    return x[:HALF] + x[HALF:]


def exchange_kernel(
    own_ref, pair_ref, left_ref, wide_high, wide_low, coulomb, out_ref, rho, za, zb, solved
):
    def column(ref, first, c, step=ROWS):
        return jnp.concatenate(
            [ref[pl.ds(first + COLS * p + c, SLABS, stride=step), :] for p in range(PLANES)], 0
        )

    def partner(d, c):
        return column(pair_ref, d * SLABS * ROWS, c)

    def place(c):
        return slice(48 * (c // 3), 48 * (c // 3) + 48), slice(128 * (c % 3), 128 * (c % 3) + 128)

    for c in range(COLS):
        own = column(own_ref, 0, c, 2 * ROWS)
        rows, cols = place(c)
        for d in range(2):
            high, low = split(own * partner(d, c))
            rho[d, rows, cols] = high
            rho[d, slice(HALF + rows.start, HALF + rows.stop), cols] = low
    for w in range(2):
        window = slice(128 * w, 128 * w + 256)
        out = None
        for d in range(2):
            both = dot(rho[d, :, window], wide_high[w, d])
            term = folded(both) + dot(rho[d, :HALF, window], wide_low[w, d])
            out = term if out is None else out + term
        for c in range(6):
            for i in range(4):
                y = 8 * c + 4 * w + i
                za[PITCH * y : PITCH * y + NG, :] = out[48 * c : 48 * c + 48, 128 * i : 128 * i + 128]

    def planes(ref, k):
        return jnp.concatenate([ref[PITCH * i : PITCH * i + NG, :] for i in (k, k + 1)], 1)

    def across(ref, k):
        return jnp.concatenate([ref[pl.ds(i, NG, stride=PITCH), :] for i in (k, k + 1)], 1)

    def put(ref, k, both):
        for e in range(2):
            ref[PITCH * (k + e) : PITCH * (k + e) + NG, :] = both[:, 128 * e : 128 * e + 128]

    for y in range(0, NG, 2):
        put(zb, y, left_mul(left_ref[0], planes(za, y)))
    for k in range(0, NG, 2):
        both = left_mul(left_ref[1], across(zb, k)) * jnp.concatenate([coulomb[k], coulomb[k + 1]], 1)
        put(za, k, left_mul(left_ref[2], both))
    for y in range(0, NG, 2):
        both = left_mul(left_ref[3], across(za, y))
        for e in range(2):
            c, w, i = (y + e) // 8, ((y + e) % 8) // 4, (y + e) % 4
            high, low = split(both[:, 128 * e : 128 * e + 128])
            solved[w, 48 * c : 48 * c + 48, 128 * i : 128 * i + 128] = high
            solved[w, HALF + 48 * c : HALF + 48 * c + 48, 128 * i : 128 * i + 128] = low
    thirds = []
    for d in range(2):
        a, b = [
            folded(dot_t(solved[w], wide_high[w, d])) + dot_t(solved[w, :HALF], wide_low[w, d]) for w in range(2)
        ]
        thirds.append((a[:, :128], a[:, 128:] + b[:, :128], b[:, 128:]))
    for c in range(COLS):
        rows, _ = place(c)
        out = thirds[0][c % 3][rows] * partner(0, c)
        out = out + thirds[1][c % 3][rows] * partner(1, c)
        for p in range(PLANES):
            out_ref[pl.ds(COLS * p + c, SLABS, stride=ROWS), :] = out[16 * p : 16 * p + 16]
    for r in range(USED, ROWS):
        out_ref[pl.ds(r, SLABS, stride=ROWS), :] = jnp.zeros((SLABS, 128), f32)


def partial_exchange(own, pair, made):
    big = pltpu.VMEM((NG * PITCH, 128), f32)
    rho, solved = pltpu.VMEM((2, 2 * HALF, 384), bf16), pltpu.VMEM((2, 2 * HALF, 512), bf16)
    return pl.pallas_call(
        exchange_kernel,
        out_shape=jax.ShapeDtypeStruct((SLABS * ROWS, 128), f32),
        scratch_shapes=[rho, big, big, solved],
        name="exchange",
        compiler_params=LARGE,
    )(own, pair, jnp.asarray(LEFTS), *made)


def prepare_kernel(slab_ref, copies_ref, tile_ref):
    tile_ref[USED:ROWS, :] = jnp.zeros((ROWS - USED, 128), f32)
    for p in range(PLANES):
        for c in range(COLS):
            r = COLS * p + c
            tile_ref[r : r + 1, :] = slab_ref[p, :, 128 * c : 128 * c + 128]
    tile = tile_ref[...]
    for k in range(CHIPS):
        copies_ref[k] = tile


def prepare(slab):
    return pl.pallas_call(
        prepare_kernel,
        out_shape=jax.ShapeDtypeStruct((CHIPS, ROWS, 128), f32),
        scratch_shapes=[pltpu.VMEM((ROWS, 128), f32)],
        name="prepare",
        compiler_params=SMALL,
    )(slab)


def role_of(xl):
    xh = lax.axis_index("xh")
    return xl + xh - 2 * xl * xh


def join_kernel(chips_ref, out_ref):
    tile = chips_ref[role_of(lax.axis_index("xl")) * 8 + lax.axis_index(("z4", "z2", "z1"))]
    for k in range(SLABS):
        out_ref[k, :ROWS, :] = tile
        out_ref[k, ROWS:, :] = chips_ref[k]


def join(chips):
    return pl.pallas_call(
        join_kernel,
        out_shape=jax.ShapeDtypeStruct((SLABS, 2 * ROWS, 128), f32),
        name="join",
        compiler_params=SMALL,
    )(chips)


def column_kernel(share_ref, orbital_ref, field_ref, copies_ref):
    field = jnp.sum(share_ref[...], axis=0)
    field_ref[...] = field
    sums = [
        jnp.sum(field * orbital_ref[ROWS * k : ROWS * k + ROWS, :], axis=0, keepdims=True) for k in range(BANDS)
    ]
    high, low = split(jnp.concatenate(sums + [jnp.zeros((128 - BANDS, 128), f32)], 0))
    ones = jnp.ones((8, 128), bf16)
    line = (dot_t(ones, high) + dot_t(ones, low))[:1]
    for k in range(SLABS):
        copies_ref[k] = line


def column_part(shares, orbitals):
    field = jax.ShapeDtypeStruct((ROWS, 128), f32)
    copies = jax.ShapeDtypeStruct((SLABS, 1, 128), f32)
    return pl.pallas_call(column_kernel, out_shape=(field, copies), name="column", compiler_params=SMALL)(
        shares, orbitals
    )


def attach_kernel(field_ref, parts_ref, copies_ref):
    column = sum(parts_ref[k] for k in range(SLABS))
    row = lax.broadcasted_iota(jnp.int32, (ROWS, 128), 0)
    tile = jnp.where(row == USED, column, field_ref[...])
    for k in range(CHIPS):
        copies_ref[k] = tile


def attach(field, parts):
    copies = jax.ShapeDtypeStruct((CHIPS, ROWS, 128), f32)
    return pl.pallas_call(attach_kernel, out_shape=copies, name="attach", compiler_params=SMALL)(field, parts)


BLOCK = 16


def place_of(band):
    return (band % 2) * CHIPS + band // 2


def finish_kernel(field_ref, out_ref, flat):
    mine = lax.axis_index(CORE + PAIR)
    starts = [ROWS * (CHIPS * core + 8 * role_of(xl)) for core in range(2) for xl in range(2)]
    matrix = jnp.concatenate([field_ref[pl.ds(start + USED, 8, stride=ROWS), :] for start in starts], 0)
    matrix = matrix[:, :BANDS]
    definite = (matrix + matrix.T) * (-0.5 / float(NG**3))
    row = lax.broadcasted_iota(jnp.int32, (BANDS, 2 * BANDS), 0)
    lane = lax.broadcasted_iota(jnp.int32, (BANDS, 2 * BANDS), 1)
    order = 2 * (row % CHIPS) + row // CHIPS
    unit = jnp.where(row[:, :BANDS] == lane[:, :BANDS], 1.0, 0.0).astype(f32)
    state = jnp.concatenate([definite, unit], 1)
    for first in range(0, BANDS, BLOCK):
        at = [place_of(first + i) for i in range(BLOCK)]
        columns = [jnp.broadcast_to(state[:, a : a + 1], (BANDS, 2 * BANDS)) for a in at]
        pivots = [state[a : a + 1, :] for a in at]
        for i in range(BLOCK):
            inverse = 1.0 / columns[i][at[i] : at[i] + 1, :]
            factor = jnp.where(order > first + i, columns[i] * inverse, 0.0)
            for j in range(i + 1, BLOCK):
                columns[j] = columns[j] - factor * columns[j][at[i] : at[i] + 1, :]
                pivots[j] = pivots[j] - factor[at[j] : at[j] + 1, :] * pivots[i]
            state = state - factor * pivots[i]
    picked = jnp.sum(jnp.where(row == mine, state, 0.0), axis=0, keepdims=True)
    pivot = jnp.sum(jnp.where(lane[:1] == mine, picked, 0.0), axis=1, keepdims=True)
    weights = picked * lax.rsqrt(pivot)
    total = None
    for k in range(BANDS):
        weight = weights[:, BANDS + k : BANDS + k + 1]
        start = pl.multiple_of(starts[k // 8] + ROWS * (k % 8), 8)
        term = weight * field_ref[pl.ds(start, ROWS), :]
        total = term if total is None else total + term
    flat[...] = total
    for p in range(PLANES):
        for c in range(COLS):
            r = COLS * p + c
            out_ref[p, :, 128 * c : 128 * c + 128] = flat[r : r + 1, :]


def finish(fields):
    return pl.pallas_call(
        finish_kernel,
        out_shape=jax.ShapeDtypeStruct((PLANES, 1, NG * NG), f32),
        scratch_shapes=[pltpu.VMEM((ROWS, 128), f32)],
        name="finish",
        compiler_params=SMALL,
    )(fields)


def exchange_tiles(tiles, axis):
    return lax.all_to_all(tiles, axis, 0, 0, tiled=True)


def exchange_roles(tiles):
    return lax.all_to_all(tiles, CROSS, 0, 0, axis_index_groups=ROLES, tiled=True)


def both_cores(chips):
    return lax.all_gather(chips, CORE, axis=0, tiled=False).reshape(-1, 128)


def per_device(orbitals):
    copies = prepare(jnp.transpose(orbitals, (1, 0, 2)))
    made = tables(jnp.asarray(LAST_HIGH), jnp.asarray(LAST_LOW))
    chips = exchange_tiles(copies, PAIR)
    whole, others = lax.optimization_barrier((exchange_roles(join(chips)), both_cores(chips)))
    pair = both_cores(whole[:, ROWS:])
    partial = partial_exchange(whole.reshape(SLABS * 2 * ROWS, 128), pair, made)
    shares = exchange_roles(partial.reshape(SLABS, ROWS, 128))
    field, lines = column_part(shares, others)
    parts = exchange_roles(lines)
    fields = both_cores(exchange_tiles(attach(field, parts), PAIR))
    return jnp.transpose(finish(fields), (1, 0, 2))


def solution(mesh):
    parted = Mesh(mesh.devices.reshape((2,) * 9), BAND + GRID)
    spec = P(BAND, GRID, None)
    return jax.shard_map(per_device, mesh=parted, in_specs=(spec,), out_specs=spec, check_vma=False)
```
